32 devices in a mesh: row: 8 (over z, x), col: 4 (over y, core).
Axes of the slice: x: 2, y: 2, z: 4, core: 2. Of those that a mesh axis runs over, the one named last changes fastest.
Arguments:
- samples: float32 [4096, 512], P(('row', 'col')), may hold values from -8 to 8
- labels: int32 [4096, 256], P(('row', 'col')), may hold values from -1 to 1, as said below
Outputs:
- statistic: float32 [256], replicated
- proof: float32 [4096], P(('row', 'col'))
- p_value: float32 [], replicated
The draws below stay inside these ranges and needn't reach their ends.
Inputs may be any that keep to these rules, and one draw needn't show every extreme that they name: `labels`: every column holds exactly 2048 entries +1 and 2048 entries -1.
All inputs are finite; a program needn't handle non-finite values.
Results may differ from the reference program's by a relative error of at most 0.0003.
Values sent between devices are 32-bit elements; how exact they have to be, the bound alone decides.
A program may use at most 64 MiB of HBM per device.

```python
import math
import jax
import jax.numpy as jnp
from jax import lax

W = 512
PERMS = 256
NS = 4096


def draw_samples(key, part):
    base = jax.random.fold_in(key, 11)
    member_key, center_key, spread_key, jitter_key, scale_key = jax.random.split(base, 5)
    member = jax.random.randint(member_key, (NS,), 0, 128)
    spread = jnp.exp(jax.random.uniform(spread_key, (128, 1), jnp.float32, jnp.log(0.7), jnp.log(2.5)))
    scales = jnp.exp(jax.random.uniform(scale_key, (NS, 1), jnp.float32, jnp.log(0.25), jnp.log(1.0)))
    centers = jnp.clip(jax.random.normal(center_key, (128, W), jnp.float32), -2.5, 2.5)
    jitter = jnp.clip(jax.random.normal(jitter_key, (NS, W), jnp.float32), -1.5, 1.5)
    placed = (centers * spread)[member]
    return (placed + jitter * scales).astype(jnp.float32)


def draw_labels(key, part):
    keys = jax.random.split(jax.random.fold_in(key, 23), PERMS)
    orders = jax.vmap(lambda one: jax.random.permutation(one, NS))(keys)
    return jnp.where(orders < NS // 2, 1, -1).astype(jnp.int32).T


def setup_inputs(seed: int = 0) -> dict:
    key_list = jax.random.split(jax.random.key(seed), 3)
    return {
        "samples": draw_samples(jax.random.fold_in(key_list[2], 71), 0),
        "labels": draw_labels(jax.random.fold_in(key_list[2], 71), 0),
    }


def tile_terms(xr, lr, gr, xc, lc, gc, width):
    norm_rows = lax.optimization_barrier(jnp.sum(xr * xr, 1))
    norm_cols = lax.optimization_barrier(jnp.sum(xc * xc, 1))
    dots = lax.dot_general(xr, xc, (((1,), (1,)), ((), ())), precision=lax.Precision.HIGHEST, preferred_element_type=jnp.float32)
    dist = jnp.maximum(norm_rows[:, None] + norm_cols[None, :] - 2.0 * dots, 0.0)
    kern = jnp.where(gr[:, None] == gc[None, :], 0.0, jnp.exp(-dist / (2.0 * width)))
    proj = jnp.dot(kern, lc, precision=lax.Precision.HIGHEST, preferred_element_type=jnp.float32)
    return (proj[:, 0], lax.optimization_barrier(jnp.sum(lr * proj, 0)), jnp.sum(kern))

def reference(samples, labels):
    total_rows = samples.shape[0]
    width = samples.shape[1]
    perms = labels.shape[1]
    labs = labels.astype(jnp.float32)
    tile = math.gcd(total_rows, 1024)
    count = total_rows // tile
    ids = jnp.arange(total_rows, dtype=jnp.int32)

    def one(args):
        xr, lr, gr = args
        return tile_terms(xr, lr, gr, samples, labs, ids, width)
    wit, quad, tot = lax.map(one, (samples.reshape(count, tile, width), labs.reshape(count, tile, perms), ids.reshape(count, tile)))
    quad = lax.optimization_barrier(jnp.sum(quad, 0))
    total = jnp.sum(tot)
    half = total_rows / 2.0
    statistic = total / (2.0 * half * (half - 1.0)) + (2.0 * half - 1.0) / (2.0 * half * (half - 1.0)) * quad
    proof = wit.reshape(total_rows) / jnp.sqrt(jnp.float32(total_rows))
    p_value = jnp.mean(jax.nn.sigmoid(4.0 * (statistic[1:] - statistic[0])))
    return (statistic, proof, p_value)
```

```python
import functools
import math

import jax
import jax.numpy as jnp
from jax import lax
from jax.experimental import pallas as pl
from jax.experimental.pallas import tpu as pltpu
from jax.sharding import PartitionSpec as P

MESH = pl.DeviceIdType.MESH
F32 = jnp.float32
BF16 = jnp.bfloat16
CHUNKS = 4
PARTS = 2
LIMIT = 60 * 1024 * 1024

ROUTES = {1: {}, 2: {0: (1, 1)}, 4: {0: (1, 3), 2: (-1, 1), 3: (-1, 2)}}


def nt(a, b):
    return lax.dot_general(a, b, (((1,), (1,)), ((), ())), preferred_element_type=F32)


def nn(a, b):
    return lax.dot_general(a, b, (((1,), (0,)), ((), ())), preferred_element_type=F32)


def split(v):
    hi = v.astype(BF16)
    return hi, (v - hi.astype(F32)).astype(BF16)


def to_row(column):
    n = column.shape[0]
    return jnp.transpose(jnp.broadcast_to(column, (n, n)))[0:1, :]


class Plan:
    def __init__(self, n_row, n_col, blk, width, perms):
        self.nz = math.gcd(n_row, 4)
        self.nx = n_row // self.nz
        self.nk = math.gcd(n_col, 2)
        self.ny = n_col // self.nk
        self.n_col = n_col
        self.n_lev = self.nx * n_col
        self.blk, self.width, self.perms = blk, width, perms
        self.direct = n_row * n_col <= 32
        self.group = math.gcd(n_col, 4)
        self.rows = blk * n_row * n_col


def kernel(pn, n_send, x_hbm, l_hbm, stat_ref, proof_ref, p_ref, x_ref, l_ref, RX, RL, CX, CL, RHI, RLO, RLB, NR,
           ROWP, PROJ, QUAD, TOT, COLP, S1, R1, S2, R2, in_sem, send, lev_sem, z_sem, s1_send, s1_recv, s2_send, s2_recv, here):
    nx, ny, nz, nk, n_col, n_lev, blk = pn.nx, pn.ny, pn.nz, pn.nk, pn.n_col, pn.n_lev, pn.blk
    row, col = lax.axis_index("row"), lax.axis_index("col")
    z, x = row // nx, row % nx
    y, core = col // nk, col % nk
    me = x * n_col + col
    routes = ROUTES[nz]
    pending = []

    def lev_of(xx, yy, kk):
        return xx * n_col + yy * nk + kk

    def dev(zz, xx, yy, kk):
        return (zz * nx + xx, yy * nk + kk)

    def lev_dev(k):
        return (z * nx + k // n_col, k % n_col)

    loads = [pltpu.make_async_copy(x_hbm, x_ref, in_sem.at[0]), pltpu.make_async_copy(l_hbm, l_ref, in_sem.at[1])]
    for c in loads:
        c.start()
    barrier = pltpu.get_barrier_semaphore()
    for d in range(1, n_lev):
        pl.semaphore_signal(barrier, inc=1, device_id=lev_dev((me + d) % n_lev), device_id_type=MESH)
    for d in range(1, nz):
        pl.semaphore_signal(barrier, inc=1, device_id=dev((z + d) % nz, x, y, core), device_id_type=MESH)
    pl.semaphore_wait(barrier, n_lev - 1 + nz - 1)
    for c in loads:
        c.wait()

    n_dev = nz * n_lev
    direct = pn.direct
    if direct:
        for d in range(1, nz):
            pl.semaphore_signal(here, inc=1, device_id=dev((z + d) % nz, x, y, core), device_id_type=MESH)

    counter = [0]

    def new_sem():
        counter[0] += 1
        return send.at[counter[0] - 1]

    half = blk // PARTS
    piece = blk // CHUNKS

    def lev_copy(k, part, target, own, sem):
        r = pl.ds(part * half, half)
        out = []
        for i, (src, dst) in enumerate(((x_ref, RX), (l_ref, RL))):
            s = src.at[r] if own else dst.at[k, r]
            out.append(pltpu.make_async_remote_copy(
                src_ref=s, dst_ref=dst.at[k, r], send_sem=new_sem() if sem else send.at[0],
                recv_sem=lev_sem.at[k, part * 2 + i], device_id=target, device_id_type=MESH))
        return out

    def lev_send(k, part, target, own=False):
        for c in lev_copy(k, part, target, own, True):
            c.start()
            pending.append(c)

    def lev_wait(k, part):
        for c in lev_copy(k, part, (row, col), False, False):
            c.wait_recv()

    def z_copy(b, ch, target, own, sems):
        r = pl.ds(ch * piece, piece)
        out = []
        for i, (src, dst) in enumerate(((x_ref, CX), (l_ref, CL))):
            s = src.at[r] if own else dst.at[b, r]
            out.append(pltpu.make_async_remote_copy(
                src_ref=s, dst_ref=dst.at[b, r], send_sem=sems[i],
                recv_sem=z_sem.at[b, ch * 2 + i], device_id=target, device_id_type=MESH))
        return out

    z_pending = []

    def z_send(b, ch, at, own):
        sems = [new_sem(), new_sem()]
        to = at + routes[b][0]

        @pl.when(z == at)
        def _():
            for c in z_copy(b, ch, dev(to, x, y, core), own, sems):
                c.start()
        z_pending.append((b, ch, at, own, sems))

    def z_arrive(b, ch, at):
        for c in z_copy(b, ch, (row, col), False, [send.at[0]] * 2):
            c.wait_recv()

    def z_round(hop, ch):
        for b in routes:
            if hop < routes[b][1]:
                at = b + routes[b][0] * hop

                @pl.when(z == at)
                def _():
                    z_arrive(b, ch, at)
                z_send(b, ch, at, False)

    def xm(d):
        return (x + d) % nx

    def ym(d):
        return (y + d) % ny

    other = (core + 1) % nk
    A, B = 0, 1
    for ch in range(CHUNKS):
        for b in routes:
            z_send(b, ch, b, True)
    for d in range(1, nx):
        lev_send(me, A, dev(z, xm(d), y, core), True)
    for d in range(1, ny):
        lev_send(me, B, dev(z, x, ym(d), core), True)
    for d in range(1, nx):
        lev_send(me, B, dev(z, xm(d), y, core), True)
    for d in range(1, ny):
        lev_send(me, A, dev(z, x, ym(d), core), True)
    if nk > 1:
        for part in (A, B):
            lev_send(me, part, dev(z, x, y, other), True)

    def prep(k, xv, lv):
        rows = pl.ds(pl.multiple_of(k * blk, blk), blk)
        hi, lo = split(xv)
        RHI[rows, :] = hi
        RLO[rows, :] = lo
        RLB[rows, :] = lv.astype(F32).astype(BF16)
        NR[:, rows] = to_row(jnp.sum(xv * xv, axis=1, keepdims=True))

    def prep_chunk(xx, skip):
        def step(i, _):
            k = xx * n_col + (col + i) % n_col
            prep(k, RX[k], RL[k])
            return 0

        lax.fori_loop(skip, n_col, step, 0)

    span = pn.group * blk
    scale = -1.0 / (2.0 * pn.width)

    def tile(slot, xx, xv, lv, own):
        chi, clo = split(xv)
        nc = jnp.sum(xv * xv, axis=1, keepdims=True)
        l0 = lv[:, 0:1].astype(F32)
        proj = PROJ[slot]
        tot = TOT[slot:slot + 1, :]
        for j in range(n_col // pn.group):
            base = pl.multiple_of(xx * n_col * blk + j * span, span)
            rows = pl.ds(base, span)
            hi, lo, lb = RHI[rows, :], RLO[rows, :], RLB[rows, :]
            dots = nt(chi, hi) + nt(chi, lo) + nt(clo, hi)
            dist = jnp.maximum(nc + NR[:, rows] - 2.0 * dots, 0.0)
            kern = jnp.exp(dist * scale)
            if own:
                ids = lax.broadcasted_iota(jnp.int32, (blk, span), 1) + base
                mine = lax.broadcasted_iota(jnp.int32, (blk, span), 0) + me * blk
                kern = jnp.where(ids == mine, 0.0, kern)
            kh, kl = split(kern)
            proj = proj + nn(kh, lb) + nn(kl, lb)
            t = jnp.sum(kern, axis=0, keepdims=True)
            for g in range(pn.group):
                tot = tot + t[:, g * blk:(g + 1) * blk]
            if not own:
                ROWP[:, rows] += jnp.sum(kern * l0, axis=0, keepdims=True)
        PROJ[slot] = proj
        TOT[slot:slot + 1, :] = tot

    def line_tiles(hop, chunks, arrive):
        for b in routes:
            if hop <= routes[b][1]:
                at = b + routes[b][0] * hop

                @pl.when(z == at)
                def _():
                    if arrive and hop == routes[b][1]:
                        for ch in range(CHUNKS):
                            z_arrive(b, ch, at)
                    for xx in chunks:
                        tile(b, xx, CX[b], CL[b], False)

    def own_tile(xx):
        tile(nz, xx, x_ref[...], l_ref[...], True)

    prep(me, x_ref[...], l_ref[...])
    ROWP[...] = jnp.zeros_like(ROWP)
    PROJ[...] = jnp.zeros_like(PROJ)
    TOT[...] = jnp.zeros_like(TOT)

    def partner(k, part):
        if nk > 1:
            lev_send(k, part, dev(z, x, y, other))

    z_round(1, 0)
    for d in range(1, nx):
        k = lev_of(xm(d), y, core)
        lev_wait(k, A)
        for e in range(1, ny):
            lev_send(k, A, dev(z, x, ym(e), core))
        partner(k, A)
    for d in range(1, ny):
        k = lev_of(x, ym(d), core)
        lev_wait(k, B)
        for e in range(1, nx):
            lev_send(k, B, dev(z, xm(e), y, core))
        partner(k, B)
    z_round(1, 1)
    z_round(2, 0)
    z_round(1, 2)
    z_round(2, 1)
    z_round(1, 3)
    for d in range(1, ny):
        k = lev_of(x, ym(d), core)
        lev_wait(k, A)
        partner(k, A)
    for d in range(1, nx):
        k = lev_of(xm(d), y, core)
        lev_wait(k, B)
        partner(k, B)
    z_round(2, 2)

    def other_core(xx, ys):
        if nk > 1:
            for e in ys:
                for part in (A, B):
                    lev_wait(lev_of(xx, ym(e), other), part)

    other_core(x, range(ny))
    prep_chunk(x, 1)
    own_tile(x)
    z_round(2, 3)
    line_tiles(1, [x], True)
    for d in range(1, nx):
        for e in range(1, ny):
            k = lev_of(xm(d), ym(e), core)
            for part in (A, B):
                lev_wait(k, part)
                partner(k, part)
    far = [xm(d) for d in range(1, nx)]
    for xx in far:
        other_core(xx, range(ny))
        prep_chunk(xx, 0)
        own_tile(xx)
    line_tiles(1, far, False)
    for hop in range(2, nz):
        line_tiles(hop, [x] + far, True)

    quad = jnp.zeros((1, pn.perms), F32)
    tot = jnp.zeros((1, blk), F32)
    for b in list(routes) + [nz]:
        w = 1.0 if b == nz else 2.0
        lv = l_ref[...] if b == nz else CL[b]
        QUAD[b:b + 1, :] = jnp.zeros((1, pn.perms), F32)
        COLP[b:b + 1, :] = jnp.zeros((1, blk), F32)
        reach = [nz - 1] if b == nz else [b + routes[b][0] * h for h in range(1, routes[b][1] + 1)]

        @pl.when((z >= (0 if b == nz else min(reach))) & (z <= max(reach)))
        def _():
            QUAD[b:b + 1, :] = w * jnp.sum(lv.astype(F32) * PROJ[b], axis=0, keepdims=True)
            COLP[b:b + 1, :] = to_row(PROJ[b][:, 0:1])
        quad = quad + QUAD[b:b + 1, :]
        tot = tot + w * TOT[b:b + 1, :]
    own_proof = COLP[nz:nz + 1, :]

    qr = pn.perms // 128
    if direct:
        def head(ref, i):
            for j in range(qr):
                ref[i, j:j + 1, :] = quad[:, j * 128:(j + 1) * 128]
            ref[i, qr:qr + 1, :] = tot

        index = z * n_lev + me
        none = jnp.zeros((1, 128), F32)
        for k in range(n_lev):
            head(S1, k)
            S1[k, qr + 1:qr + 2, :] = ROWP[:, k * blk:(k + 1) * blk]
        for b in range(nz):
            head(S2, b)
            S2[b, qr + 1:qr + 2, :] = COLP[b:b + 1, :] if b in routes else none
        head(S2, nz)
        S2[nz, qr + 1:qr + 2, :] = none
        if nz > 1:
            pl.semaphore_wait(here, nz - 1)

        def x_copy(dz, d, slot):
            b, k = (z + dz) % nz, (me + d) % n_lev
            src = S1.at[k] if dz == 0 else (S2.at[b] if d == 0 else S2.at[nz])
            return pltpu.make_async_remote_copy(
                src_ref=src, dst_ref=R1.at[slot], send_sem=s1_send.at[dz * n_lev + d], recv_sem=s1_recv.at[slot],
                device_id=(b * nx + k // n_col, k % n_col), device_id_type=MESH)

        pairs = [(dz, d) for dz in reversed(range(nz)) for d in range(n_lev) if dz + d > 0]
        for dz, d in pairs:
            x_copy(dz, d, index).start()
        R1[index] = S1[me]
        for dz, d in pairs:
            x_copy(dz, d, ((z + dz) % nz) * n_lev + (me + d) % n_lev).wait_recv()
        done = R1[0]
        for i in range(1, n_dev):
            done = done + R1[i]
        proof = done[qr + 1:qr + 2, :] + own_proof
    else:
        for k in range(n_lev):
            for i in range(qr):
                S1[k, i:i + 1, :] = quad[:, i * 128:(i + 1) * 128]
            S1[k, qr:qr + 1, :] = tot
            S1[k, qr + 1:qr + 2, :] = ROWP[:, k * blk:(k + 1) * blk]

        def s1_copy(d):
            k = (me + d) % n_lev
            return pltpu.make_async_remote_copy(
                src_ref=S1.at[k], dst_ref=R1.at[me], send_sem=s1_send.at[k], recv_sem=s1_recv.at[me],
                device_id=lev_dev(k), device_id_type=MESH)

        def s1_in(d):
            k = (me + d) % n_lev
            return pltpu.make_async_remote_copy(
                src_ref=S1.at[k], dst_ref=R1.at[k], send_sem=s1_send.at[k], recv_sem=s1_recv.at[k],
                device_id=lev_dev(k), device_id_type=MESH)

        for d in range(1, n_lev):
            s1_copy(d).start()
        acc = S1[me]
        for d in range(1, n_lev):
            s1_in(d).wait_recv()
            acc = acc + R1[(me + d) % n_lev]
        for b in range(nz):
            S2[b, :, :] = acc
            S2[b, qr + 1:qr + 2, :] = COLP[b:b + 1, :] if b in routes else jnp.zeros((1, 128), F32)

        def s2_copy(d):
            b = (z + d) % nz
            return pltpu.make_async_remote_copy(
                src_ref=S2.at[b], dst_ref=R2.at[z], send_sem=s2_send.at[b], recv_sem=s2_recv.at[z],
                device_id=dev(b, x, y, core), device_id_type=MESH)

        def s2_in(d):
            b = (z + d) % nz
            return pltpu.make_async_remote_copy(
                src_ref=S2.at[b], dst_ref=R2.at[b], send_sem=s2_send.at[b], recv_sem=s2_recv.at[b],
                device_id=dev(b, x, y, core), device_id_type=MESH)

        for d in range(1, nz):
            s2_copy(d).start()
        for d in range(1, nz):
            s2_in(d).wait_recv()
        tops = []
        extra = jnp.zeros((1, 128), F32)
        for b in range(nz):
            mine = z == b
            tops.append(jnp.where(mine, acc, R2[b]))
            extra = extra + jnp.where(mine, 0.0, R2[b, qr + 1:qr + 2, :])
        done = functools.reduce(lambda u, v: u + v, tops)
        proof = acc[qr + 1:qr + 2, :] + own_proof + extra
    total = jnp.sum(done[qr:qr + 1, :], axis=1, keepdims=True)
    hf = pn.rows / 2.0
    den = 2.0 * hf * (hf - 1.0)
    stat = total / den + ((2.0 * hf - 1.0) / den) * done[0:qr, :]
    stat_ref[...] = stat
    proof_ref[...] = proof / math.sqrt(pn.rows)
    sg = 1.0 / (1.0 + jnp.exp(-4.0 * (stat - stat[0:1, 0:1])))
    first = (lax.broadcasted_iota(jnp.int32, stat.shape, 0) + lax.broadcasted_iota(jnp.int32, stat.shape, 1)) == 0
    sg = jnp.where(first, 0.0, sg)
    p = jnp.sum(jnp.sum(sg, axis=0, keepdims=True), axis=1, keepdims=True) / (pn.perms - 1)
    p_ref[...] = p

    for c in pending:
        c.wait_send()
    for b, ch, at, own, sems in z_pending:
        @pl.when(z == at)
        def _():
            for c in z_copy(b, ch, dev(at + routes[b][0], x, y, core), own, sems):
                c.wait_send()
    if direct:
        for dz, d in pairs:
            x_copy(dz, d, index).wait_send()
    else:
        for d in range(1, n_lev):
            s1_copy(d).wait_send()
        for d in range(1, nz):
            s2_copy(d).wait_send()
    assert counter[0] == n_send


def send_count(pn):
    nx, ny, nk, nz = pn.nx, pn.ny, pn.nk, pn.nz
    own = 2 * (nx - 1) + 2 * (ny - 1) + (2 if nk > 1 else 0)
    fwd = 2 * (nx - 1) * (ny - 1)
    core = 2 * (nx * ny - 1) if nk > 1 else 0
    line = sum(h for _, h in ROUTES[nz].values()) * CHUNKS
    return 2 * (own + fwd + core + line)


def line_kernel(x_hbm, l_hbm, out_ref, x_ref, l_ref, GX, GL, CX, CL, CC, HI, LO, LB, NR, NC, L0, OWN0,
                ROWP, PROJ, TOT, S1, S2, R1, in_sem, xy_send, xy_recv, z_send, z_recv, m_send, m_recv, line, here):
    blk, width = x_ref.shape
    perms = l_ref.shape[1]
    nx, ny, nk, nz, n_lev = 2, 2, 2, 4, 8
    row, col = lax.axis_index("row"), lax.axis_index("col")
    z, x = row // nx, row % nx
    y, core = col // nk, col % nk
    qr = perms // 128
    OWN = 4
    A, B = 0, 1

    def dev(zz, xx, yy, kk):
        return (zz * nx + xx, yy * nk + kk)

    def signal(sem, to):
        pl.semaphore_signal(sem, inc=1, device_id=to, device_id_type=MESH)

    def remote(src, dst, ss, rs, to):
        return pltpu.make_async_remote_copy(src_ref=src, dst_ref=dst, send_sem=ss, recv_sem=rs, device_id=to,
                                            device_id_type=MESH)

    here_dev = (row, col)
    x_dev, y_dev, k_dev = dev(z, 1 - x, y, core), dev(z, x, 1 - y, core), dev(z, x, y, 1 - core)
    place = [(xx, yy, kk) for xx, yy, kk in ((x, y, core), (x, y, 1 - core), (1 - x, y, core), (x, 1 - y, core),
             (1 - x, y, 1 - core), (x, 1 - y, 1 - core), (1 - x, 1 - y, core), (1 - x, 1 - y, 1 - core))]

    loads = [pltpu.make_async_copy(x_hbm, x_ref, in_sem.at[0]), pltpu.make_async_copy(l_hbm, l_ref, in_sem.at[1])]
    for c in loads:
        c.start()
    barrier = pltpu.get_barrier_semaphore()
    for to in (x_dev, y_dev, k_dev):
        signal(barrier, to)

    @pl.when(z > 0)
    def _():
        signal(barrier, dev(z - 1, x, y, core))

    @pl.when(z < nz - 1)
    def _():
        signal(barrier, dev(z + 1, x, y, core))

    ROWP[...] = jnp.zeros_like(ROWP)
    PROJ[...] = jnp.zeros_like(PROJ)
    TOT[...] = jnp.zeros_like(TOT)
    for c in reversed(loads):
        c.wait()
    OWN0[...] = to_row(l_ref[:, 0:1].astype(F32)).astype(jnp.int32)
    pl.semaphore_wait(barrier, 3 + jnp.where(z > 0, 1, 0) + jnp.where(z < nz - 1, 1, 0))

    half = blk // 2

    def xy_copy(src, dst, part, i, to):
        r = pl.ds(part * half, half)
        mine, buf = ((x_ref, GX), (l_ref, GL))[i]
        s = mine.at[r] if src == 0 else buf.at[src, r]
        n = part * 2 + i
        return remote(s, buf.at[dst, r], xy_send.at[dst, n], xy_recv.at[dst, n], to)

    sent = []
    X, L = 0, 1

    def xy_start(src, dst, part, to, kinds=(X, L)):
        for i in kinds:
            c = xy_copy(src, dst, part, i, to)
            c.start()
            sent.append(c)

    def xy_wait(at, parts=(A, B), kinds=(X, L)):
        for part in parts:
            for i in kinds:
                xy_copy(at, at, part, i, here_dev).wait_recv()

    piece = blk // 4
    SAM, LAB = [0, 1, 2, 3], [5, 6, 7, 8]

    def z_copy(b, p, own, to):
        if p == 4:
            src, dst = (OWN0 if own else CC.at[b]), CC.at[b]
        else:
            r = pl.ds((p if p < 4 else p - 5) * piece, piece)
            mine, buf = (x_ref, CX) if p < 4 else (l_ref, CL)
            src, dst = (mine.at[r] if own else buf.at[b, r]), buf.at[b, r]
        return remote(src, dst, z_send.at[b, p], z_recv.at[b, p], to)

    def z_start(b, ps, own, step):
        for p in ps:
            z_copy(b, p, own, dev(z + step, x, y, core)).start()

    def z_wait(b, ps):
        for p in ps:
            z_copy(b, p, False, here_dev).wait_recv()

    def z_pass(b, ps, step):
        for p in ps:
            z_wait(b, [p])
            z_start(b, [p], False, step)

    def at_z(*levels):
        cond = z == levels[0]
        for v in levels[1:]:
            cond = cond | (z == v)
        return pl.when(cond)

    @at_z(0)
    def _():
        z_start(0, SAM + [4] + LAB, True, 1)

    @at_z(2)
    def _():
        z_start(2, SAM + [4], True, -1)
        signal(line, dev(1, x, y, core))

    @at_z(3)
    def _():
        z_start(3, SAM + [4] + LAB, True, -1)

    @at_z(1)
    def _():
        signal(line, dev(2, x, y, core))

    xy_start(0, 2, A, x_dev)
    xy_start(0, 3, B, y_dev)
    xy_start(0, 2, B, x_dev)
    xy_start(0, 3, A, y_dev)
    xy_start(0, 1, A, k_dev)
    xy_start(0, 1, B, k_dev)

    scale = -1.0 / (2.0 * width)
    span = nk * blk

    def put(at, v):
        hi, lo = split(v)
        rows = slice(at, at + blk)
        HI[rows, :] = hi
        LO[rows, :] = lo
        return jnp.sum(v * v, axis=1, keepdims=True)

    def prep(at, v, lv):
        n = put(at * blk, v)
        rows = slice(at * blk, (at + 1) * blk)
        LB[rows, :] = lv.astype(F32).astype(BF16)
        NR[:, rows] = to_row(n)
        return n

    def prep_at(at):
        prep(at, GX[at], GL[at])

    def prep_line(b):
        NC[b] = put((n_lev + b) * blk, CX[b])
        L0[b] = jnp.transpose(jnp.broadcast_to(CC[b], (blk, blk)))[:, 0:1].astype(F32)

    def slot_of(j):
        return jnp.where(j == 0, OWN, jnp.where(j == 1, jnp.where(z == 2, 3, 0),
                         jnp.where(j == 2, jnp.where(z == 1, 2, 0), 3)))

    def unit(j, g):
        s = slot_of(j)
        own = s == OWN
        c = pl.ds(pl.multiple_of(jnp.where(own, 0, n_lev + s) * blk, blk), blk)
        rows = pl.ds(pl.multiple_of(g * span, span), span)
        chi, clo = HI[c, :], LO[c, :]
        hi, lo, lb = HI[rows, :], LO[rows, :], LB[rows, :]
        dots = nt(chi, hi) + nt(chi, lo) + nt(clo, hi)
        dist = jnp.maximum(NC[s] + NR[:, rows] - 2.0 * dots, 0.0)
        kern = jnp.exp(dist * scale)
        gap = lax.broadcasted_iota(jnp.int32, kern.shape, 1) - lax.broadcasted_iota(jnp.int32, kern.shape, 0)
        kern = jnp.where(gap == jnp.where(own & (g == 0), 0, n_lev * blk), 0.0, kern)
        kh, kl = split(kern)
        PROJ[s] += nn(kh, lb) + nn(kl, lb)
        t = jnp.sum(kern, axis=0, keepdims=True)
        w = jnp.where(own, 1.0, 2.0)
        TOT[...] += w * (t[:, :blk] + t[:, blk:])
        ROWP[:, rows] += jnp.sum(kern * L0[s], axis=0, keepdims=True)

    def units(j0, j1, g0, g1):
        def outer(j, _):
            def inner(g, _):
                unit(j, g)
                return 0
            lax.fori_loop(g0, g1, inner, 0)
            return 0
        lax.fori_loop(j0, j1, outer, 0)

    early = jnp.where(z == 0, 1, 4 - z)
    every = jnp.where(z == 0, 1, 5 - z)
    NC[OWN] = prep(0, x_ref[...], l_ref[...])
    L0[OWN] = jnp.zeros((blk, 1), F32)
    xy_wait(1)
    prep_at(1)
    units(0, 1, 0, 1)

    @at_z(1)
    def _():
        z_pass(0, [0, 1], 1)
        pl.semaphore_wait(line, 1)
        signal(line, dev(0, x, y, core))
        z_pass(0, [2], 1)

    @at_z(2)
    def _():
        z_pass(3, [0, 1], -1)
        pl.semaphore_wait(line, 1)
        signal(line, dev(3, x, y, core))
        z_pass(3, [2], -1)

    xy_wait(2, (A,))
    xy_start(2, 6, A, y_dev)
    xy_start(2, 4, A, k_dev)
    xy_wait(3, (B,))
    xy_start(3, 6, B, x_dev)
    xy_start(3, 5, B, k_dev)

    @at_z(1)
    def _():
        z_pass(0, [3, 4], 1)
        prep_line(0)
        z_wait(2, SAM + [4])
        prep_line(2)

    @at_z(2)
    def _():
        z_pass(3, [3, 4], -1)
        z_start(2, LAB, True, -1)
        prep_line(3)
        z_pass(0, [0], 1)

    units(1, early, 0, 1)

    @at_z(1)
    def _():
        z_pass(0, LAB, 1)

    @at_z(2)
    def _():
        z_pass(0, [1], 1)
        z_pass(3, LAB[:3], -1)
        z_pass(0, [2], 1)
        z_pass(3, LAB[3:], -1)

    xy_wait(2, (B,))
    xy_start(2, 4, B, k_dev)
    xy_wait(3, (A,))
    xy_start(3, 5, A, k_dev)
    prep_at(2)
    prep_at(3)
    units(0, early, 1, 2)

    @at_z(2)
    def _():
        z_pass(0, [3, 4], 1)
        prep_line(0)

    xy_wait(4)
    xy_wait(5)
    prep_at(4)
    prep_at(5)
    units(0, early, 2, 3)

    @at_z(2)
    def _():
        z_pass(0, LAB[:2], 1)

    for part in (A, B):
        xy_wait(6, (part,), (X,))
        xy_start(6, 7, part, k_dev, (X,))

    @at_z(1)
    def _():
        z_wait(3, SAM + [4])
        prep_line(3)

    @at_z(1, 2)
    def _():
        units(early, every, 0, 1)

    for part in (A, B):
        xy_wait(6, (part,), (L,))
        xy_start(6, 7, part, k_dev, (L,))

    @at_z(2)
    def _():
        z_pass(0, LAB[2:], 1)

    @at_z(3)
    def _():
        z_wait(0, SAM + [4])
        prep_line(0)

    @at_z(0, 3)
    def _():
        pl.semaphore_wait(line, 1)

    units(early, every, jnp.where(z == 3, 0, 1), 3)
    prep_at(6)
    xy_wait(7)
    for xx, yy, kk in place[1:]:
        signal(here, dev(z, xx, yy, kk))
    prep_at(7)
    units(0, every, 3, 4)

    none = jnp.zeros((1, 128), F32)
    own_proof = to_row(PROJ[OWN][:, 0:1])
    tot = TOT[...]
    for i in range(n_lev):
        S1[i, qr:qr + 1, :] = tot
        S1[i, qr + 1:qr + 2, :] = ROWP[:, i * blk:(i + 1) * blk]
    for b in range(nz + 1):
        S2[b, qr:qr + 1, :] = tot
        S2[b, qr + 1:qr + 2, :] = to_row(PROJ[b][:, 0:1]) if b in (0, 2, 3) else none

    def quad_of(s, lv):
        return jnp.sum(lv.astype(F32) * PROJ[s], axis=0, keepdims=True)

    def add(q):
        for j in range(qr):
            S2[nz, j:j + 1, :] += q[:, j * 128:(j + 1) * 128]

    S2[nz, 0:qr, :] = jnp.zeros((qr, 128), F32)
    add(quad_of(OWN, l_ref[...]))

    @at_z(3)
    def _():
        z_wait(0, LAB)

    @at_z(1, 2, 3)
    def _():
        add(2.0 * quad_of(0, CL[0]))

    @at_z(1)
    def _():
        z_wait(2, LAB)
        add(2.0 * quad_of(2, CL[2]))
        z_wait(3, LAB)

    @at_z(1, 2)
    def _():
        add(2.0 * quad_of(3, CL[3]))

    q = S2[nz, 0:qr, :]
    for i in range(n_lev):
        S1[i, 0:qr, :] = q
    for b in range(nz):
        S2[b, 0:qr, :] = q
    index = z * n_lev + x * 4 + col
    pl.semaphore_wait(here, n_lev - 1)

    def m_copy(dz, i, incoming):
        b = (z + dz) % nz
        xx, yy, kk = place[i]
        src = S1.at[i] if dz == 0 else (S2.at[b] if i == 0 else S2.at[nz])
        slot = b * n_lev + xx * 4 + yy * nk + kk if incoming else index
        return remote(src, R1.at[slot], m_send.at[dz * n_lev + i], m_recv.at[slot], dev(b, xx, yy, kk))

    pairs = [(dz, i) for dz in reversed(range(nz)) for i in range(n_lev) if dz + i > 0]
    for dz, i in pairs:
        m_copy(dz, i, False).start()
    R1[index] = S1[0]
    for dz, i in pairs:
        m_copy(dz, i, True).wait_recv()
    done = R1[0]
    for i in range(1, nz * n_lev):
        done = done + R1[i]
    out_ref[0:qr + 1, :] = done[0:qr + 1, :]
    out_ref[qr + 1:qr + 2, :] = done[qr + 1:qr + 2, :] + own_proof

    for c in sent:
        c.wait_send()
    for at, b in ((0, 0), (1, 0), (2, 0), (2, 2), (2, 3), (3, 3)):
        @at_z(at)
        def _():
            for p in SAM + [4] + LAB:
                z_copy(b, p, False, here_dev).wait_send()
    for dz, i in pairs:
        m_copy(dz, i, False).wait_send()


def finish(rows, perms, r_ref, stat_ref, proof_ref, p_ref):
    qr = perms // 128
    total = jnp.sum(r_ref[qr:qr + 1, :], axis=1, keepdims=True)
    hf = rows / 2.0
    den = 2.0 * hf * (hf - 1.0)
    stat = total / den + ((2.0 * hf - 1.0) / den) * r_ref[0:qr, :]
    stat_ref[...] = stat
    proof_ref[...] = r_ref[qr + 1:qr + 2, :] / math.sqrt(rows)
    sg = 1.0 / (1.0 + jnp.exp(-4.0 * (stat - stat[0:1, 0:1])))
    first = (lax.broadcasted_iota(jnp.int32, stat.shape, 0) + lax.broadcasted_iota(jnp.int32, stat.shape, 1)) == 0
    sg = jnp.where(first, 0.0, sg)
    p_ref[...] = jnp.sum(jnp.sum(sg, axis=0, keepdims=True), axis=1, keepdims=True) / (perms - 1)


def line_call(samples, labels):
    blk, width = samples.shape
    perms = labels.shape[1]
    qr = perms // 128
    nz, n_lev = 4, 8
    slots = nz * n_lev
    i32 = jnp.int32
    dma = pltpu.SemaphoreType.DMA
    vm = pl.BlockSpec(memory_space=pltpu.VMEM)
    hbm = pl.BlockSpec(memory_space=pl.ANY)
    res = pl.pallas_call(
        line_kernel,
        out_shape=jax.ShapeDtypeStruct((qr + 2, 128), F32),
        in_specs=[hbm, hbm],
        out_specs=vm,
        scratch_shapes=[
            pltpu.VMEM((blk, width), F32),
            pltpu.VMEM((blk, perms), i32),
            pltpu.VMEM((n_lev, blk, width), F32),
            pltpu.VMEM((n_lev, blk, perms), i32),
            pltpu.VMEM((nz, blk, width), F32),
            pltpu.VMEM((nz, blk, perms), i32),
            pltpu.VMEM((nz, 1, blk), i32),
            pltpu.VMEM(((n_lev + nz) * blk, width), BF16),
            pltpu.VMEM(((n_lev + nz) * blk, width), BF16),
            pltpu.VMEM((n_lev * blk, perms), BF16),
            pltpu.VMEM((1, n_lev * blk), F32),
            pltpu.VMEM((nz + 1, blk, 1), F32),
            pltpu.VMEM((nz + 1, blk, 1), F32),
            pltpu.VMEM((1, blk), i32),
            pltpu.VMEM((1, n_lev * blk), F32),
            pltpu.VMEM((nz + 1, blk, perms), F32),
            pltpu.VMEM((1, blk), F32),
            pltpu.VMEM((n_lev, qr + 2, 128), F32),
            pltpu.VMEM((nz + 1, qr + 2, 128), F32),
            pltpu.VMEM((slots, qr + 2, 128), F32),
            dma((2,)),
            dma((n_lev, 4)),
            dma((n_lev, 4)),
            dma((nz, 9)),
            dma((nz, 9)),
            dma((slots,)),
            dma((slots,)),
            pltpu.SemaphoreType.REGULAR,
            pltpu.SemaphoreType.REGULAR,
        ],
        compiler_params=pltpu.CompilerParams(
            collective_id=1, has_side_effects=True, vmem_limit_bytes=LIMIT
        ),
    )(samples, labels)
    return pl.pallas_call(
        functools.partial(finish, blk * slots, perms),
        out_shape=(
            jax.ShapeDtypeStruct((qr, 128), F32),
            jax.ShapeDtypeStruct((1, blk), F32),
            jax.ShapeDtypeStruct((1, 1), F32),
        ),
        in_specs=[vm],
        out_specs=(vm, vm, vm),
    )(res)


def solution(mesh):
    n_row, n_col = mesh.shape["row"], mesh.shape["col"]

    def shards(samples, labels):
        blk, width = samples.shape
        perms = labels.shape[1]
        pn = Plan(n_row, n_col, blk, width, perms)
        n_send = send_count(pn)
        n_lev, nz = pn.n_lev, pn.nz
        if (pn.nx, pn.ny, pn.nk, nz, blk) == (2, 2, 2, 4, 128):
            stat, proof, p = line_call(samples, labels)
            return stat.reshape(perms), proof.reshape(blk), p.reshape(())
        msg = perms // 128 + 2
        slots = n_row * n_col if pn.direct else n_lev
        vm = pl.BlockSpec(memory_space=pltpu.VMEM)
        hbm = pl.BlockSpec(memory_space=pl.ANY)
        dma = pltpu.SemaphoreType.DMA
        stat, proof, p = pl.pallas_call(
            functools.partial(kernel, pn, n_send),
            out_shape=(
                jax.ShapeDtypeStruct((perms // 128, 128), F32),
                jax.ShapeDtypeStruct((1, blk), F32),
                jax.ShapeDtypeStruct((1, 1), F32),
            ),
            in_specs=[hbm, hbm],
            out_specs=(vm, vm, vm),
            scratch_shapes=[
                pltpu.VMEM((blk, width), F32),
                pltpu.VMEM((blk, perms), jnp.int32),
                pltpu.VMEM((n_lev, blk, width), F32),
                pltpu.VMEM((n_lev, blk, perms), jnp.int32),
                pltpu.VMEM((nz, blk, width), F32),
                pltpu.VMEM((nz, blk, perms), jnp.int32),
                pltpu.VMEM((n_lev * blk, width), BF16),
                pltpu.VMEM((n_lev * blk, width), BF16),
                pltpu.VMEM((n_lev * blk, perms), BF16),
                pltpu.VMEM((1, n_lev * blk), F32),
                pltpu.VMEM((1, n_lev * blk), F32),
                pltpu.VMEM((nz + 1, blk, perms), F32),
                pltpu.VMEM((nz + 1, perms), F32),
                pltpu.VMEM((nz + 1, blk), F32),
                pltpu.VMEM((nz + 1, blk), F32),
                pltpu.VMEM((n_lev, msg, 128), F32),
                pltpu.VMEM((slots, msg, 128), F32),
                pltpu.VMEM((nz + 1, msg, 128), F32),
                pltpu.VMEM((nz, msg, 128), F32),
                dma((2,)),
                dma((n_send,)),
                dma((n_lev, 2 * PARTS)),
                dma((nz, 2 * CHUNKS)),
                dma((slots,)),
                dma((slots,)),
                dma((nz,)),
                dma((nz,)),
                pltpu.SemaphoreType.REGULAR,
            ],
            compiler_params=pltpu.CompilerParams(
                collective_id=0, has_side_effects=True, vmem_limit_bytes=60 * 1024 * 1024
            ),
        )(samples, labels)
        return stat.reshape(perms), proof.reshape(blk), p.reshape(())

    placed = (P(("row", "col"), None), P(("row", "col"), None))
    return jax.shard_map(
        shards, mesh=mesh, in_specs=placed, out_specs=(P(), P(("row", "col")), P()), check_vma=False
    )
```

```python
import functools
import math

import jax
import jax.numpy as jnp
from jax import lax
from jax.experimental import pallas as pl
from jax.experimental.pallas import tpu as pltpu
from jax.sharding import PartitionSpec as P

MESH = pl.DeviceIdType.MESH
F32 = jnp.float32
BF16 = jnp.bfloat16
CHUNKS = 4
PARTS = 2
LIMIT = 60 * 1024 * 1024

ROUTES = {1: {}, 2: {0: (1, 1)}, 4: {0: (1, 3), 2: (-1, 1), 3: (-1, 2)}}


def nt(a, b):
    return lax.dot_general(a, b, (((1,), (1,)), ((), ())), preferred_element_type=F32)


def nn(a, b):
    return lax.dot_general(a, b, (((1,), (0,)), ((), ())), preferred_element_type=F32)


def split(v):
    hi = v.astype(BF16)
    return hi, (v - hi.astype(F32)).astype(BF16)


def to_row(column):
    n = column.shape[0]
    return jnp.transpose(jnp.broadcast_to(column, (n, n)))[0:1, :]


class Plan:
    def __init__(self, n_row, n_col, blk, width, perms):
        self.nz = math.gcd(n_row, 4)
        self.nx = n_row // self.nz
        self.nk = math.gcd(n_col, 2)
        self.ny = n_col // self.nk
        self.n_col = n_col
        self.n_lev = self.nx * n_col
        self.blk, self.width, self.perms = blk, width, perms
        self.direct = n_row * n_col <= 32
        self.group = math.gcd(n_col, 4)
        self.rows = blk * n_row * n_col


def kernel(pn, n_send, x_hbm, l_hbm, stat_ref, proof_ref, p_ref, x_ref, l_ref, RX, RL, CX, CL, RHI, RLO, RLB, NR,
           ROWP, PROJ, QUAD, TOT, COLP, S1, R1, S2, R2, in_sem, send, lev_sem, z_sem, s1_send, s1_recv, s2_send, s2_recv, here):
    nx, ny, nz, nk, n_col, n_lev, blk = pn.nx, pn.ny, pn.nz, pn.nk, pn.n_col, pn.n_lev, pn.blk
    row, col = lax.axis_index("row"), lax.axis_index("col")
    z, x = row // nx, row % nx
    y, core = col // nk, col % nk
    me = x * n_col + col
    routes = ROUTES[nz]
    pending = []

    def lev_of(xx, yy, kk):
        return xx * n_col + yy * nk + kk

    def dev(zz, xx, yy, kk):
        return (zz * nx + xx, yy * nk + kk)

    def lev_dev(k):
        return (z * nx + k // n_col, k % n_col)

    loads = [pltpu.make_async_copy(x_hbm, x_ref, in_sem.at[0]), pltpu.make_async_copy(l_hbm, l_ref, in_sem.at[1])]
    for c in loads:
        c.start()
    barrier = pltpu.get_barrier_semaphore()
    for d in range(1, n_lev):
        pl.semaphore_signal(barrier, inc=1, device_id=lev_dev((me + d) % n_lev), device_id_type=MESH)
    for d in range(1, nz):
        pl.semaphore_signal(barrier, inc=1, device_id=dev((z + d) % nz, x, y, core), device_id_type=MESH)
    pl.semaphore_wait(barrier, n_lev - 1 + nz - 1)
    for c in loads:
        c.wait()

    n_dev = nz * n_lev
    direct = pn.direct
    if direct:
        for d in range(1, nz):
            pl.semaphore_signal(here, inc=1, device_id=dev((z + d) % nz, x, y, core), device_id_type=MESH)

    counter = [0]

    def new_sem():
        counter[0] += 1
        return send.at[counter[0] - 1]

    half = blk // PARTS
    piece = blk // CHUNKS

    def lev_copy(k, part, target, own, sem):
        r = pl.ds(part * half, half)
        out = []
        for i, (src, dst) in enumerate(((x_ref, RX), (l_ref, RL))):
            s = src.at[r] if own else dst.at[k, r]
            out.append(pltpu.make_async_remote_copy(
                src_ref=s, dst_ref=dst.at[k, r], send_sem=new_sem() if sem else send.at[0],
                recv_sem=lev_sem.at[k, part * 2 + i], device_id=target, device_id_type=MESH))
        return out

    def lev_send(k, part, target, own=False):
        for c in lev_copy(k, part, target, own, True):
            c.start()
            pending.append(c)

    def lev_wait(k, part):
        for c in lev_copy(k, part, (row, col), False, False):
            c.wait_recv()

    def z_copy(b, ch, target, own, sems):
        r = pl.ds(ch * piece, piece)
        out = []
        for i, (src, dst) in enumerate(((x_ref, CX), (l_ref, CL))):
            s = src.at[r] if own else dst.at[b, r]
            out.append(pltpu.make_async_remote_copy(
                src_ref=s, dst_ref=dst.at[b, r], send_sem=sems[i],
                recv_sem=z_sem.at[b, ch * 2 + i], device_id=target, device_id_type=MESH))
        return out

    z_pending = []

    def z_send(b, ch, at, own):
        sems = [new_sem(), new_sem()]
        to = at + routes[b][0]

        @pl.when(z == at)
        def _():
            for c in z_copy(b, ch, dev(to, x, y, core), own, sems):
                c.start()
        z_pending.append((b, ch, at, own, sems))

    def z_arrive(b, ch, at):
        for c in z_copy(b, ch, (row, col), False, [send.at[0]] * 2):
            c.wait_recv()

    def z_round(hop, ch):
        for b in routes:
            if hop < routes[b][1]:
                at = b + routes[b][0] * hop

                @pl.when(z == at)
                def _():
                    z_arrive(b, ch, at)
                z_send(b, ch, at, False)

    def xm(d):
        return (x + d) % nx

    def ym(d):
        return (y + d) % ny

    other = (core + 1) % nk
    A, B = 0, 1
    for ch in range(CHUNKS):
        for b in routes:
            z_send(b, ch, b, True)
    for d in range(1, nx):
        lev_send(me, A, dev(z, xm(d), y, core), True)
    for d in range(1, ny):
        lev_send(me, B, dev(z, x, ym(d), core), True)
    for d in range(1, nx):
        lev_send(me, B, dev(z, xm(d), y, core), True)
    for d in range(1, ny):
        lev_send(me, A, dev(z, x, ym(d), core), True)
    if nk > 1:
        for part in (A, B):
            lev_send(me, part, dev(z, x, y, other), True)

    def prep(k, xv, lv):
        rows = pl.ds(pl.multiple_of(k * blk, blk), blk)
        hi, lo = split(xv)
        RHI[rows, :] = hi
        RLO[rows, :] = lo
        RLB[rows, :] = lv.astype(F32).astype(BF16)
        NR[:, rows] = to_row(jnp.sum(xv * xv, axis=1, keepdims=True))

    def prep_chunk(xx, skip):
        def step(i, _):
            k = xx * n_col + (col + i) % n_col
            prep(k, RX[k], RL[k])
            return 0

        lax.fori_loop(skip, n_col, step, 0)

    span = pn.group * blk
    scale = -1.0 / (2.0 * pn.width)

    def tile(slot, xx, xv, lv, own):
        chi, clo = split(xv)
        nc = jnp.sum(xv * xv, axis=1, keepdims=True)
        l0 = lv[:, 0:1].astype(F32)
        proj = PROJ[slot]
        tot = TOT[slot:slot + 1, :]
        for j in range(n_col // pn.group):
            base = pl.multiple_of(xx * n_col * blk + j * span, span)
            rows = pl.ds(base, span)
            hi, lo, lb = RHI[rows, :], RLO[rows, :], RLB[rows, :]
            dots = nt(chi, hi) + nt(chi, lo) + nt(clo, hi)
            dist = jnp.maximum(nc + NR[:, rows] - 2.0 * dots, 0.0)
            kern = jnp.exp(dist * scale)
            if own:
                ids = lax.broadcasted_iota(jnp.int32, (blk, span), 1) + base
                mine = lax.broadcasted_iota(jnp.int32, (blk, span), 0) + me * blk
                kern = jnp.where(ids == mine, 0.0, kern)
            kh, kl = split(kern)
            proj = proj + nn(kh, lb) + nn(kl, lb)
            t = jnp.sum(kern, axis=0, keepdims=True)
            for g in range(pn.group):
                tot = tot + t[:, g * blk:(g + 1) * blk]
            if not own:
                ROWP[:, rows] += jnp.sum(kern * l0, axis=0, keepdims=True)
        PROJ[slot] = proj
        TOT[slot:slot + 1, :] = tot

    def line_tiles(hop, chunks, arrive):
        for b in routes:
            if hop <= routes[b][1]:
                at = b + routes[b][0] * hop

                @pl.when(z == at)
                def _():
                    if arrive and hop == routes[b][1]:
                        for ch in range(CHUNKS):
                            z_arrive(b, ch, at)
                    for xx in chunks:
                        tile(b, xx, CX[b], CL[b], False)

    def own_tile(xx):
        tile(nz, xx, x_ref[...], l_ref[...], True)

    prep(me, x_ref[...], l_ref[...])
    ROWP[...] = jnp.zeros_like(ROWP)
    PROJ[...] = jnp.zeros_like(PROJ)
    TOT[...] = jnp.zeros_like(TOT)

    def partner(k, part):
        if nk > 1:
            lev_send(k, part, dev(z, x, y, other))

    z_round(1, 0)
    for d in range(1, nx):
        k = lev_of(xm(d), y, core)
        lev_wait(k, A)
        for e in range(1, ny):
            lev_send(k, A, dev(z, x, ym(e), core))
        partner(k, A)
    for d in range(1, ny):
        k = lev_of(x, ym(d), core)
        lev_wait(k, B)
        for e in range(1, nx):
            lev_send(k, B, dev(z, xm(e), y, core))
        partner(k, B)
    z_round(1, 1)
    z_round(2, 0)
    z_round(1, 2)
    z_round(2, 1)
    z_round(1, 3)
    for d in range(1, ny):
        k = lev_of(x, ym(d), core)
        lev_wait(k, A)
        partner(k, A)
    for d in range(1, nx):
        k = lev_of(xm(d), y, core)
        lev_wait(k, B)
        partner(k, B)
    z_round(2, 2)

    def other_core(xx, ys):
        if nk > 1:
            for e in ys:
                for part in (A, B):
                    lev_wait(lev_of(xx, ym(e), other), part)

    other_core(x, range(ny))
    prep_chunk(x, 1)
    own_tile(x)
    z_round(2, 3)
    line_tiles(1, [x], True)
    for d in range(1, nx):
        for e in range(1, ny):
            k = lev_of(xm(d), ym(e), core)
            for part in (A, B):
                lev_wait(k, part)
                partner(k, part)
    far = [xm(d) for d in range(1, nx)]
    for xx in far:
        other_core(xx, range(ny))
        prep_chunk(xx, 0)
        own_tile(xx)
    line_tiles(1, far, False)
    for hop in range(2, nz):
        line_tiles(hop, [x] + far, True)

    quad = jnp.zeros((1, pn.perms), F32)
    tot = jnp.zeros((1, blk), F32)
    for b in list(routes) + [nz]:
        w = 1.0 if b == nz else 2.0
        lv = l_ref[...] if b == nz else CL[b]
        QUAD[b:b + 1, :] = jnp.zeros((1, pn.perms), F32)
        COLP[b:b + 1, :] = jnp.zeros((1, blk), F32)
        reach = [nz - 1] if b == nz else [b + routes[b][0] * h for h in range(1, routes[b][1] + 1)]

        @pl.when((z >= (0 if b == nz else min(reach))) & (z <= max(reach)))
        def _():
            QUAD[b:b + 1, :] = w * jnp.sum(lv.astype(F32) * PROJ[b], axis=0, keepdims=True)
            COLP[b:b + 1, :] = to_row(PROJ[b][:, 0:1])
        quad = quad + QUAD[b:b + 1, :]
        tot = tot + w * TOT[b:b + 1, :]
    own_proof = COLP[nz:nz + 1, :]

    qr = pn.perms // 128
    if direct:
        def head(ref, i):
            for j in range(qr):
                ref[i, j:j + 1, :] = quad[:, j * 128:(j + 1) * 128]
            ref[i, qr:qr + 1, :] = tot

        index = z * n_lev + me
        none = jnp.zeros((1, 128), F32)
        for k in range(n_lev):
            head(S1, k)
            S1[k, qr + 1:qr + 2, :] = ROWP[:, k * blk:(k + 1) * blk]
        for b in range(nz):
            head(S2, b)
            S2[b, qr + 1:qr + 2, :] = COLP[b:b + 1, :] if b in routes else none
        head(S2, nz)
        S2[nz, qr + 1:qr + 2, :] = none
        if nz > 1:
            pl.semaphore_wait(here, nz - 1)

        def x_copy(dz, d, slot):
            b, k = (z + dz) % nz, (me + d) % n_lev
            src = S1.at[k] if dz == 0 else (S2.at[b] if d == 0 else S2.at[nz])
            return pltpu.make_async_remote_copy(
                src_ref=src, dst_ref=R1.at[slot], send_sem=s1_send.at[dz * n_lev + d], recv_sem=s1_recv.at[slot],
                device_id=(b * nx + k // n_col, k % n_col), device_id_type=MESH)

        pairs = [(dz, d) for dz in reversed(range(nz)) for d in range(n_lev) if dz + d > 0]
        for dz, d in pairs:
            x_copy(dz, d, index).start()
        R1[index] = S1[me]
        for dz, d in pairs:
            x_copy(dz, d, ((z + dz) % nz) * n_lev + (me + d) % n_lev).wait_recv()
        done = R1[0]
        for i in range(1, n_dev):
            done = done + R1[i]
        proof = done[qr + 1:qr + 2, :] + own_proof
    else:
        for k in range(n_lev):
            for i in range(qr):
                S1[k, i:i + 1, :] = quad[:, i * 128:(i + 1) * 128]
            S1[k, qr:qr + 1, :] = tot
            S1[k, qr + 1:qr + 2, :] = ROWP[:, k * blk:(k + 1) * blk]

        def s1_copy(d):
            k = (me + d) % n_lev
            return pltpu.make_async_remote_copy(
                src_ref=S1.at[k], dst_ref=R1.at[me], send_sem=s1_send.at[k], recv_sem=s1_recv.at[me],
                device_id=lev_dev(k), device_id_type=MESH)

        def s1_in(d):
            k = (me + d) % n_lev
            return pltpu.make_async_remote_copy(
                src_ref=S1.at[k], dst_ref=R1.at[k], send_sem=s1_send.at[k], recv_sem=s1_recv.at[k],
                device_id=lev_dev(k), device_id_type=MESH)

        for d in range(1, n_lev):
            s1_copy(d).start()
        acc = S1[me]
        for d in range(1, n_lev):
            s1_in(d).wait_recv()
            acc = acc + R1[(me + d) % n_lev]
        for b in range(nz):
            S2[b, :, :] = acc
            S2[b, qr + 1:qr + 2, :] = COLP[b:b + 1, :] if b in routes else jnp.zeros((1, 128), F32)

        def s2_copy(d):
            b = (z + d) % nz
            return pltpu.make_async_remote_copy(
                src_ref=S2.at[b], dst_ref=R2.at[z], send_sem=s2_send.at[b], recv_sem=s2_recv.at[z],
                device_id=dev(b, x, y, core), device_id_type=MESH)

        def s2_in(d):
            b = (z + d) % nz
            return pltpu.make_async_remote_copy(
                src_ref=S2.at[b], dst_ref=R2.at[b], send_sem=s2_send.at[b], recv_sem=s2_recv.at[b],
                device_id=dev(b, x, y, core), device_id_type=MESH)

        for d in range(1, nz):
            s2_copy(d).start()
        for d in range(1, nz):
            s2_in(d).wait_recv()
        tops = []
        extra = jnp.zeros((1, 128), F32)
        for b in range(nz):
            mine = z == b
            tops.append(jnp.where(mine, acc, R2[b]))
            extra = extra + jnp.where(mine, 0.0, R2[b, qr + 1:qr + 2, :])
        done = functools.reduce(lambda u, v: u + v, tops)
        proof = acc[qr + 1:qr + 2, :] + own_proof + extra
    total = jnp.sum(done[qr:qr + 1, :], axis=1, keepdims=True)
    hf = pn.rows / 2.0
    den = 2.0 * hf * (hf - 1.0)
    stat = total / den + ((2.0 * hf - 1.0) / den) * done[0:qr, :]
    stat_ref[...] = stat
    proof_ref[...] = proof / math.sqrt(pn.rows)
    sg = 1.0 / (1.0 + jnp.exp(-4.0 * (stat - stat[0:1, 0:1])))
    first = (lax.broadcasted_iota(jnp.int32, stat.shape, 0) + lax.broadcasted_iota(jnp.int32, stat.shape, 1)) == 0
    sg = jnp.where(first, 0.0, sg)
    p = jnp.sum(jnp.sum(sg, axis=0, keepdims=True), axis=1, keepdims=True) / (pn.perms - 1)
    p_ref[...] = p

    for c in pending:
        c.wait_send()
    for b, ch, at, own, sems in z_pending:
        @pl.when(z == at)
        def _():
            for c in z_copy(b, ch, dev(at + routes[b][0], x, y, core), own, sems):
                c.wait_send()
    if direct:
        for dz, d in pairs:
            x_copy(dz, d, index).wait_send()
    else:
        for d in range(1, n_lev):
            s1_copy(d).wait_send()
        for d in range(1, nz):
            s2_copy(d).wait_send()
    assert counter[0] == n_send


def send_count(pn):
    nx, ny, nk, nz = pn.nx, pn.ny, pn.nk, pn.nz
    own = 2 * (nx - 1) + 2 * (ny - 1) + (2 if nk > 1 else 0)
    fwd = 2 * (nx - 1) * (ny - 1)
    core = 2 * (nx * ny - 1) if nk > 1 else 0
    line = sum(h for _, h in ROUTES[nz].values()) * CHUNKS
    return 2 * (own + fwd + core + line)


def line_kernel(x_hbm, l_hbm, out_ref, x_ref, l_ref, GX, GL, CX, CL, CC, HI, LO, LB, SH, SL, NR, NC, L0, OWN0,
                ROWP, PROJ, TOT, S1, S2, R1, in_sem, xy_send, xy_recv, z_send, z_recv, m_send, m_recv, line, here):
    blk, width = x_ref.shape
    perms = l_ref.shape[1]
    nx, ny, nk, nz, n_lev = 2, 2, 2, 4, 8
    row, col = lax.axis_index("row"), lax.axis_index("col")
    z, x = row // nx, row % nx
    y, core = col // nk, col % nk
    qr = perms // 128
    A, B = 0, 1

    def dev(zz, xx, yy, kk):
        return (zz * nx + xx, yy * nk + kk)

    def signal(sem, to):
        pl.semaphore_signal(sem, inc=1, device_id=to, device_id_type=MESH)

    def remote(src, dst, ss, rs, to):
        return pltpu.make_async_remote_copy(src_ref=src, dst_ref=dst, send_sem=ss, recv_sem=rs, device_id=to,
                                            device_id_type=MESH)

    here_dev = (row, col)
    x_dev, y_dev, k_dev = dev(z, 1 - x, y, core), dev(z, x, 1 - y, core), dev(z, x, y, 1 - core)
    place = [(xx, yy, kk) for xx, yy, kk in ((x, y, core), (x, y, 1 - core), (1 - x, y, core), (x, 1 - y, core),
             (1 - x, y, 1 - core), (x, 1 - y, 1 - core), (1 - x, 1 - y, core), (1 - x, 1 - y, 1 - core))]

    loads = [pltpu.make_async_copy(x_hbm, x_ref, in_sem.at[0]), pltpu.make_async_copy(l_hbm, l_ref, in_sem.at[1])]
    for c in loads:
        c.start()
    barrier = pltpu.get_barrier_semaphore()
    for to in (x_dev, y_dev, k_dev):
        signal(barrier, to)

    @pl.when(z > 0)
    def _():
        signal(barrier, dev(z - 1, x, y, core))

    @pl.when(z < nz - 1)
    def _():
        signal(barrier, dev(z + 1, x, y, core))

    ROWP[...] = jnp.zeros_like(ROWP)
    PROJ[...] = jnp.zeros_like(PROJ)
    TOT[...] = jnp.zeros_like(TOT)
    for c in reversed(loads):
        c.wait()
    OWN0[...] = to_row(l_ref[:, 0:1].astype(F32)).astype(jnp.int32)
    pl.semaphore_wait(barrier, 3 + jnp.where(z > 0, 1, 0) + jnp.where(z < nz - 1, 1, 0))

    half = blk // 2

    def xy_copy(src, dst, part, i, to):
        r = pl.ds(part * half, half)
        mine, buf = ((x_ref, GX), (l_ref, GL))[i]
        s = mine.at[r] if src == 0 else buf.at[src, r]
        n = part * 2 + i
        return remote(s, buf.at[dst, r], xy_send.at[dst, n], xy_recv.at[dst, n], to)

    sent = []
    X, L = 0, 1

    def xy_start(src, dst, part, to, kinds=(X, L)):
        for i in kinds:
            c = xy_copy(src, dst, part, i, to)
            c.start()
            sent.append(c)

    def xy_wait(at, parts=(A, B), kinds=(X, L)):
        for part in parts:
            for i in kinds:
                xy_copy(at, at, part, i, here_dev).wait_recv()

    piece = blk // 4
    SAM, LAB = [0, 1, 2, 3], [5, 6, 7, 8]

    def z_copy(b, p, own, to):
        if p == 4:
            src, dst = (OWN0 if own else CC.at[b]), CC.at[b]
        else:
            r = pl.ds((p if p < 4 else p - 5) * piece, piece)
            mine, buf = (x_ref, CX) if p < 4 else (l_ref, CL)
            src, dst = (mine.at[r] if own else buf.at[b, r]), buf.at[b, r]
        return remote(src, dst, z_send.at[b, p], z_recv.at[b, p], to)

    def z_start(b, ps, own, step):
        for p in ps:
            z_copy(b, p, own, dev(z + step, x, y, core)).start()

    def z_wait(b, ps):
        for p in ps:
            z_copy(b, p, False, here_dev).wait_recv()

    def z_pass(b, ps, step):
        for p in ps:
            z_wait(b, [p])
            z_start(b, [p], False, step)

    def at_z(*levels):
        cond = z == levels[0]
        for v in levels[1:]:
            cond = cond | (z == v)
        return pl.when(cond)

    @at_z(0)
    def _():
        z_start(0, SAM + [4] + LAB, True, 1)

    @at_z(2)
    def _():
        z_start(2, SAM + [4], True, -1)
        signal(line, dev(1, x, y, core))

    @at_z(3)
    def _():
        z_start(3, SAM + [4] + LAB, True, -1)

    @at_z(1)
    def _():
        signal(line, dev(2, x, y, core))

    xy_start(0, 2, A, x_dev)
    xy_start(0, 3, B, y_dev)
    xy_start(0, 2, B, x_dev)
    xy_start(0, 3, A, y_dev)
    xy_start(0, 1, A, k_dev)
    xy_start(0, 1, B, k_dev)

    scale = -1.0 / (2.0 * width)
    span = nk * blk

    order = {0: [], 1: [0, 2, 3], 2: [3, 0], 3: [0]}

    def norms(v):
        return jnp.sum(v * v, axis=1, keepdims=True)

    def prep(at, v, lv):
        hi, lo = split(v)
        n = norms(v)
        rows = slice(at * blk, (at + 1) * blk)
        HI[rows, :] = hi
        LO[rows, :] = lo
        LB[rows, :] = lv.astype(F32).astype(BF16)
        NR[:, rows] = to_row(n)
        if at == 0:
            SH[rows, :] = hi
            SL[rows, :] = lo
            NC[rows, :] = n

    def prep_at(at):
        prep(at, GX[at], GL[at])

    def prep_line(b, j):
        hi, lo = split(CX[b])
        rows = slice(j * blk, (j + 1) * blk)
        SH[rows, :] = hi
        SL[rows, :] = lo
        NC[rows, :] = norms(CX[b])
        L0[rows, :] = jnp.transpose(jnp.broadcast_to(CC[b], (blk, blk)))[:, 0:1].astype(F32)

    def work(j0, j1, *groups):
        mine = slice(j0 * blk, j1 * blk)
        n = (j1 - j0) * blk
        tiles = []
        for g in groups:
            rows = slice(g * span, (g + 1) * span)
            hi = SH[mine, :]
            d = nt(jnp.concatenate([hi, SL[mine, :]], axis=0), HI[rows, :])
            tiles.append((g, rows, d[:n] + d[n:] + nt(hi, LO[rows, :])))
        for g, rows, dots in tiles:
            dist = jnp.maximum(NC[mine, :] + NR[:, rows] - 2.0 * dots, 0.0)
            kern = jnp.exp(dist * scale)
            if j0 == 0:
                top = kern[:blk]
                if g == 0:
                    gap = lax.broadcasted_iota(jnp.int32, top.shape, 1) - lax.broadcasted_iota(jnp.int32, top.shape, 0)
                    top = jnp.where(gap == 0, 0.0, top)
                    kern = top if n == blk else jnp.concatenate([top, kern[blk:]], axis=0)
                t = jnp.sum(top, axis=0, keepdims=True)
            else:
                t = jnp.zeros((1, span), F32)
            kh, kl = split(kern)
            p = nn(jnp.concatenate([kh, kl], axis=0), LB[rows, :])
            PROJ[mine, :] += p[:n] + p[n:]
            rest = kern[blk:] if j0 == 0 else kern
            if rest.shape[0]:
                t = t + 2.0 * jnp.sum(rest, axis=0, keepdims=True)
                line_rows = slice(max(j0, 1) * blk, j1 * blk)
                ROWP[:, rows] += jnp.sum(rest * L0[line_rows, :], axis=0, keepdims=True)
            TOT[...] += t[:, :blk] + t[:, blk:]

    prep(0, x_ref[...], l_ref[...])
    xy_wait(1)
    prep_at(1)

    @at_z(0, 3)
    def _():
        work(0, 1, 0)

    @at_z(1)
    def _():
        z_pass(0, [0, 1], 1)
        pl.semaphore_wait(line, 1)
        signal(line, dev(0, x, y, core))
        z_pass(0, [2], 1)

    @at_z(2)
    def _():
        z_pass(3, [0, 1], -1)
        pl.semaphore_wait(line, 1)
        signal(line, dev(3, x, y, core))
        z_pass(3, [2], -1)

    xy_wait(2, (A,))
    xy_start(2, 6, A, y_dev)
    xy_start(2, 4, A, k_dev)
    xy_wait(3, (B,))
    xy_start(3, 6, B, x_dev)
    xy_start(3, 5, B, k_dev)

    @at_z(1)
    def _():
        z_pass(0, [3, 4], 1)
        prep_line(0, 1)
        z_wait(2, SAM + [4])
        prep_line(2, 2)
        work(0, 3, 0)
        z_pass(0, LAB, 1)

    @at_z(2)
    def _():
        z_pass(3, [3, 4], -1)
        z_start(2, LAB, True, -1)
        prep_line(3, 1)
        z_pass(0, [0], 1)
        work(0, 2, 0)
        z_pass(0, [1], 1)
        z_pass(3, LAB[:3], -1)
        z_pass(0, [2], 1)
        z_pass(3, LAB[3:], -1)

    xy_wait(2, (B,))
    xy_start(2, 4, B, k_dev)
    xy_wait(3, (A,))
    xy_start(3, 5, A, k_dev)
    prep_at(2)
    prep_at(3)

    @at_z(0, 3)
    def _():
        work(0, 1, 1)

    @at_z(1)
    def _():
        work(0, 3, 1)

    @at_z(2)
    def _():
        work(0, 2, 1)
        z_pass(0, [3, 4], 1)
        prep_line(0, 2)

    xy_wait(4)
    xy_wait(5)
    prep_at(4)
    prep_at(5)

    @at_z(0, 3)
    def _():
        work(0, 1, 2)

    @at_z(1)
    def _():
        work(0, 3, 2)

    @at_z(2)
    def _():
        work(0, 2, 2)
        z_pass(0, LAB[:2], 1)

    for part in (A, B):
        xy_wait(6, (part,), (X,))
        xy_start(6, 7, part, k_dev, (X,))

    @at_z(1)
    def _():
        z_wait(3, SAM + [4])
        prep_line(3, 3)
        work(3, 4, 0, 1, 2)

    for part in (A, B):
        xy_wait(6, (part,), (L,))
        xy_start(6, 7, part, k_dev, (L,))

    @at_z(2)
    def _():
        z_pass(0, LAB[2:], 1)
        work(2, 3, 0, 1, 2)

    @at_z(3)
    def _():
        z_wait(0, SAM + [4])
        prep_line(0, 1)
        work(1, 2, 0, 1, 2)

    @at_z(0, 3)
    def _():
        pl.semaphore_wait(line, 1)

    prep_at(6)
    xy_wait(7)
    for xx, yy, kk in place[1:]:
        signal(here, dev(z, xx, yy, kk))
    prep_at(7)
    for level in range(nz):
        @at_z(level)
        def _():
            work(0, 1 + len(order[level]), 3)

    def proj(j):
        return PROJ[j * blk:(j + 1) * blk, :]

    none = jnp.zeros((1, 128), F32)
    own_proof = to_row(proj(0)[:, 0:1])
    tot = TOT[...]
    for i in range(n_lev):
        S1[i, qr:qr + 1, :] = tot
        S1[i, qr + 1:qr + 2, :] = ROWP[:, i * blk:(i + 1) * blk]
    for b in range(nz + 1):
        S2[b, qr:qr + 1, :] = tot
        S2[b, qr + 1:qr + 2, :] = none
    for level in range(1, nz):
        @at_z(level)
        def _():
            for j, b in enumerate(order[level]):
                S2[b, qr + 1:qr + 2, :] = to_row(proj(j + 1)[:, 0:1])

    def add(w, j, lv):
        q = w * jnp.sum(lv.astype(F32) * proj(j), axis=0, keepdims=True)
        for i in range(qr):
            S2[nz, i:i + 1, :] += q[:, i * 128:(i + 1) * 128]

    S2[nz, 0:qr, :] = jnp.zeros((qr, 128), F32)
    add(1.0, 0, l_ref[...])

    @at_z(3)
    def _():
        z_wait(0, LAB)

    @at_z(1, 3)
    def _():
        add(2.0, 1, CL[0])

    @at_z(2)
    def _():
        add(2.0, 1, CL[3])
        add(2.0, 2, CL[0])

    @at_z(1)
    def _():
        z_wait(2, LAB)
        add(2.0, 2, CL[2])
        z_wait(3, LAB)
        add(2.0, 3, CL[3])

    q = S2[nz, 0:qr, :]
    for i in range(n_lev):
        S1[i, 0:qr, :] = q
    for b in range(nz):
        S2[b, 0:qr, :] = q
    index = z * n_lev + x * 4 + col
    pl.semaphore_wait(here, n_lev - 1)

    def m_copy(dz, i, incoming):
        b = (z + dz) % nz
        xx, yy, kk = place[i]
        src = S1.at[i] if dz == 0 else (S2.at[b] if i == 0 else S2.at[nz])
        slot = b * n_lev + xx * 4 + yy * nk + kk if incoming else index
        return remote(src, R1.at[slot], m_send.at[dz * n_lev + i], m_recv.at[slot], dev(b, xx, yy, kk))

    pairs = [(dz, i) for dz in reversed(range(nz)) for i in range(n_lev) if dz + i > 0]
    for dz, i in pairs:
        m_copy(dz, i, False).start()
    R1[index] = S1[0]
    for dz, i in pairs:
        m_copy(dz, i, True).wait_recv()
    done = R1[0]
    for i in range(1, nz * n_lev):
        done = done + R1[i]
    out_ref[0:qr + 1, :] = done[0:qr + 1, :]
    out_ref[qr + 1:qr + 2, :] = done[qr + 1:qr + 2, :] + own_proof

    for c in sent:
        c.wait_send()
    for at, b in ((0, 0), (1, 0), (2, 0), (2, 2), (2, 3), (3, 3)):
        @at_z(at)
        def _():
            for p in SAM + [4] + LAB:
                z_copy(b, p, False, here_dev).wait_send()
    for dz, i in pairs:
        m_copy(dz, i, False).wait_send()


def finish(rows, perms, r_ref, stat_ref, proof_ref, p_ref):
    qr = perms // 128
    total = jnp.sum(r_ref[qr:qr + 1, :], axis=1, keepdims=True)
    hf = rows / 2.0
    den = 2.0 * hf * (hf - 1.0)
    stat = total / den + ((2.0 * hf - 1.0) / den) * r_ref[0:qr, :]
    stat_ref[...] = stat
    proof_ref[...] = r_ref[qr + 1:qr + 2, :] / math.sqrt(rows)
    sg = 1.0 / (1.0 + jnp.exp(-4.0 * (stat - stat[0:1, 0:1])))
    first = (lax.broadcasted_iota(jnp.int32, stat.shape, 0) + lax.broadcasted_iota(jnp.int32, stat.shape, 1)) == 0
    sg = jnp.where(first, 0.0, sg)
    p_ref[...] = jnp.sum(jnp.sum(sg, axis=0, keepdims=True), axis=1, keepdims=True) / (perms - 1)


def line_call(samples, labels):
    blk, width = samples.shape
    perms = labels.shape[1]
    qr = perms // 128
    nz, n_lev = 4, 8
    slots = nz * n_lev
    i32 = jnp.int32
    dma = pltpu.SemaphoreType.DMA
    vm = pl.BlockSpec(memory_space=pltpu.VMEM)
    hbm = pl.BlockSpec(memory_space=pl.ANY)
    res = pl.pallas_call(
        line_kernel,
        out_shape=jax.ShapeDtypeStruct((qr + 2, 128), F32),
        in_specs=[hbm, hbm],
        out_specs=vm,
        scratch_shapes=[
            pltpu.VMEM((blk, width), F32),
            pltpu.VMEM((blk, perms), i32),
            pltpu.VMEM((n_lev, blk, width), F32),
            pltpu.VMEM((n_lev, blk, perms), i32),
            pltpu.VMEM((nz, blk, width), F32),
            pltpu.VMEM((nz, blk, perms), i32),
            pltpu.VMEM((nz, 1, blk), i32),
            pltpu.VMEM((n_lev * blk, width), BF16),
            pltpu.VMEM((n_lev * blk, width), BF16),
            pltpu.VMEM((n_lev * blk, perms), BF16),
            pltpu.VMEM((nz * blk, width), BF16),
            pltpu.VMEM((nz * blk, width), BF16),
            pltpu.VMEM((1, n_lev * blk), F32),
            pltpu.VMEM((nz * blk, 1), F32),
            pltpu.VMEM((nz * blk, 1), F32),
            pltpu.VMEM((1, blk), i32),
            pltpu.VMEM((1, n_lev * blk), F32),
            pltpu.VMEM((nz * blk, perms), F32),
            pltpu.VMEM((1, blk), F32),
            pltpu.VMEM((n_lev, qr + 2, 128), F32),
            pltpu.VMEM((nz + 1, qr + 2, 128), F32),
            pltpu.VMEM((slots, qr + 2, 128), F32),
            dma((2,)),
            dma((n_lev, 4)),
            dma((n_lev, 4)),
            dma((nz, 9)),
            dma((nz, 9)),
            dma((slots,)),
            dma((slots,)),
            pltpu.SemaphoreType.REGULAR,
            pltpu.SemaphoreType.REGULAR,
        ],
        compiler_params=pltpu.CompilerParams(
            collective_id=1, has_side_effects=True, vmem_limit_bytes=LIMIT
        ),
    )(samples, labels)
    return pl.pallas_call(
        functools.partial(finish, blk * slots, perms),
        out_shape=(
            jax.ShapeDtypeStruct((qr, 128), F32),
            jax.ShapeDtypeStruct((1, blk), F32),
            jax.ShapeDtypeStruct((1, 1), F32),
        ),
        in_specs=[vm],
        out_specs=(vm, vm, vm),
    )(res)


def solution(mesh):
    n_row, n_col = mesh.shape["row"], mesh.shape["col"]

    def shards(samples, labels):
        blk, width = samples.shape
        perms = labels.shape[1]
        pn = Plan(n_row, n_col, blk, width, perms)
        n_send = send_count(pn)
        n_lev, nz = pn.n_lev, pn.nz
        if (pn.nx, pn.ny, pn.nk, nz, blk) == (2, 2, 2, 4, 128):
            stat, proof, p = line_call(samples, labels)
            return stat.reshape(perms), proof.reshape(blk), p.reshape(())
        msg = perms // 128 + 2
        slots = n_row * n_col if pn.direct else n_lev
        vm = pl.BlockSpec(memory_space=pltpu.VMEM)
        hbm = pl.BlockSpec(memory_space=pl.ANY)
        dma = pltpu.SemaphoreType.DMA
        stat, proof, p = pl.pallas_call(
            functools.partial(kernel, pn, n_send),
            out_shape=(
                jax.ShapeDtypeStruct((perms // 128, 128), F32),
                jax.ShapeDtypeStruct((1, blk), F32),
                jax.ShapeDtypeStruct((1, 1), F32),
            ),
            in_specs=[hbm, hbm],
            out_specs=(vm, vm, vm),
            scratch_shapes=[
                pltpu.VMEM((blk, width), F32),
                pltpu.VMEM((blk, perms), jnp.int32),
                pltpu.VMEM((n_lev, blk, width), F32),
                pltpu.VMEM((n_lev, blk, perms), jnp.int32),
                pltpu.VMEM((nz, blk, width), F32),
                pltpu.VMEM((nz, blk, perms), jnp.int32),
                pltpu.VMEM((n_lev * blk, width), BF16),
                pltpu.VMEM((n_lev * blk, width), BF16),
                pltpu.VMEM((n_lev * blk, perms), BF16),
                pltpu.VMEM((1, n_lev * blk), F32),
                pltpu.VMEM((1, n_lev * blk), F32),
                pltpu.VMEM((nz + 1, blk, perms), F32),
                pltpu.VMEM((nz + 1, perms), F32),
                pltpu.VMEM((nz + 1, blk), F32),
                pltpu.VMEM((nz + 1, blk), F32),
                pltpu.VMEM((n_lev, msg, 128), F32),
                pltpu.VMEM((slots, msg, 128), F32),
                pltpu.VMEM((nz + 1, msg, 128), F32),
                pltpu.VMEM((nz, msg, 128), F32),
                dma((2,)),
                dma((n_send,)),
                dma((n_lev, 2 * PARTS)),
                dma((nz, 2 * CHUNKS)),
                dma((slots,)),
                dma((slots,)),
                dma((nz,)),
                dma((nz,)),
                pltpu.SemaphoreType.REGULAR,
            ],
            compiler_params=pltpu.CompilerParams(
                collective_id=0, has_side_effects=True, vmem_limit_bytes=60 * 1024 * 1024
            ),
        )(samples, labels)
        return stat.reshape(perms), proof.reshape(blk), p.reshape(())

    placed = (P(("row", "col"), None), P(("row", "col"), None))
    return jax.shard_map(
        shards, mesh=mesh, in_specs=placed, out_specs=(P(), P(("row", "col")), P()), check_vma=False
    )
```

```python
import functools
import math

import jax
import jax.numpy as jnp
from jax import lax
from jax.experimental import pallas as pl
from jax.experimental.pallas import tpu as pltpu
from jax.sharding import PartitionSpec as P

MESH = pl.DeviceIdType.MESH
F32 = jnp.float32
BF16 = jnp.bfloat16
CHUNKS = 4
PARTS = 2
LIMIT = 60 * 1024 * 1024

ROUTES = {1: {}, 2: {0: (1, 1)}, 4: {0: (1, 3), 2: (-1, 1), 3: (-1, 2)}}


def nt(a, b):
    return lax.dot_general(a, b, (((1,), (1,)), ((), ())), preferred_element_type=F32)


def nn(a, b):
    return lax.dot_general(a, b, (((1,), (0,)), ((), ())), preferred_element_type=F32)


def split(v):
    hi = v.astype(BF16)
    return hi, (v - hi.astype(F32)).astype(BF16)


def to_row(column):
    n = column.shape[0]
    return jnp.transpose(jnp.broadcast_to(column, (n, n)))[0:1, :]


class Plan:
    def __init__(self, n_row, n_col, blk, width, perms):
        self.nz = math.gcd(n_row, 4)
        self.nx = n_row // self.nz
        self.nk = math.gcd(n_col, 2)
        self.ny = n_col // self.nk
        self.n_col = n_col
        self.n_lev = self.nx * n_col
        self.blk, self.width, self.perms = blk, width, perms
        self.direct = n_row * n_col <= 32
        self.group = math.gcd(n_col, 4)
        self.rows = blk * n_row * n_col


def kernel(pn, n_send, x_hbm, l_hbm, stat_ref, proof_ref, p_ref, x_ref, l_ref, RX, RL, CX, CL, RHI, RLO, RLB, NR,
           ROWP, PROJ, QUAD, TOT, COLP, S1, R1, S2, R2, in_sem, send, lev_sem, z_sem, s1_send, s1_recv, s2_send, s2_recv, here):
    nx, ny, nz, nk, n_col, n_lev, blk = pn.nx, pn.ny, pn.nz, pn.nk, pn.n_col, pn.n_lev, pn.blk
    row, col = lax.axis_index("row"), lax.axis_index("col")
    z, x = row // nx, row % nx
    y, core = col // nk, col % nk
    me = x * n_col + col
    routes = ROUTES[nz]
    pending = []

    def lev_of(xx, yy, kk):
        return xx * n_col + yy * nk + kk

    def dev(zz, xx, yy, kk):
        return (zz * nx + xx, yy * nk + kk)

    def lev_dev(k):
        return (z * nx + k // n_col, k % n_col)

    loads = [pltpu.make_async_copy(x_hbm, x_ref, in_sem.at[0]), pltpu.make_async_copy(l_hbm, l_ref, in_sem.at[1])]
    for c in loads:
        c.start()
    barrier = pltpu.get_barrier_semaphore()
    for d in range(1, n_lev):
        pl.semaphore_signal(barrier, inc=1, device_id=lev_dev((me + d) % n_lev), device_id_type=MESH)
    for d in range(1, nz):
        pl.semaphore_signal(barrier, inc=1, device_id=dev((z + d) % nz, x, y, core), device_id_type=MESH)
    pl.semaphore_wait(barrier, n_lev - 1 + nz - 1)
    for c in loads:
        c.wait()

    n_dev = nz * n_lev
    direct = pn.direct
    if direct:
        for d in range(1, nz):
            pl.semaphore_signal(here, inc=1, device_id=dev((z + d) % nz, x, y, core), device_id_type=MESH)

    counter = [0]

    def new_sem():
        counter[0] += 1
        return send.at[counter[0] - 1]

    half = blk // PARTS
    piece = blk // CHUNKS

    def lev_copy(k, part, target, own, sem):
        r = pl.ds(part * half, half)
        out = []
        for i, (src, dst) in enumerate(((x_ref, RX), (l_ref, RL))):
            s = src.at[r] if own else dst.at[k, r]
            out.append(pltpu.make_async_remote_copy(
                src_ref=s, dst_ref=dst.at[k, r], send_sem=new_sem() if sem else send.at[0],
                recv_sem=lev_sem.at[k, part * 2 + i], device_id=target, device_id_type=MESH))
        return out

    def lev_send(k, part, target, own=False):
        for c in lev_copy(k, part, target, own, True):
            c.start()
            pending.append(c)

    def lev_wait(k, part):
        for c in lev_copy(k, part, (row, col), False, False):
            c.wait_recv()

    def z_copy(b, ch, target, own, sems):
        r = pl.ds(ch * piece, piece)
        out = []
        for i, (src, dst) in enumerate(((x_ref, CX), (l_ref, CL))):
            s = src.at[r] if own else dst.at[b, r]
            out.append(pltpu.make_async_remote_copy(
                src_ref=s, dst_ref=dst.at[b, r], send_sem=sems[i],
                recv_sem=z_sem.at[b, ch * 2 + i], device_id=target, device_id_type=MESH))
        return out

    z_pending = []

    def z_send(b, ch, at, own):
        sems = [new_sem(), new_sem()]
        to = at + routes[b][0]

        @pl.when(z == at)
        def _():
            for c in z_copy(b, ch, dev(to, x, y, core), own, sems):
                c.start()
        z_pending.append((b, ch, at, own, sems))

    def z_arrive(b, ch, at):
        for c in z_copy(b, ch, (row, col), False, [send.at[0]] * 2):
            c.wait_recv()

    def z_round(hop, ch):
        for b in routes:
            if hop < routes[b][1]:
                at = b + routes[b][0] * hop

                @pl.when(z == at)
                def _():
                    z_arrive(b, ch, at)
                z_send(b, ch, at, False)

    def xm(d):
        return (x + d) % nx

    def ym(d):
        return (y + d) % ny

    other = (core + 1) % nk
    A, B = 0, 1
    for ch in range(CHUNKS):
        for b in routes:
            z_send(b, ch, b, True)
    for d in range(1, nx):
        lev_send(me, A, dev(z, xm(d), y, core), True)
    for d in range(1, ny):
        lev_send(me, B, dev(z, x, ym(d), core), True)
    for d in range(1, nx):
        lev_send(me, B, dev(z, xm(d), y, core), True)
    for d in range(1, ny):
        lev_send(me, A, dev(z, x, ym(d), core), True)
    if nk > 1:
        for part in (A, B):
            lev_send(me, part, dev(z, x, y, other), True)

    def prep(k, xv, lv):
        rows = pl.ds(pl.multiple_of(k * blk, blk), blk)
        hi, lo = split(xv)
        RHI[rows, :] = hi
        RLO[rows, :] = lo
        RLB[rows, :] = lv.astype(F32).astype(BF16)
        NR[:, rows] = to_row(jnp.sum(xv * xv, axis=1, keepdims=True))

    def prep_chunk(xx, skip):
        def step(i, _):
            k = xx * n_col + (col + i) % n_col
            prep(k, RX[k], RL[k])
            return 0

        lax.fori_loop(skip, n_col, step, 0)

    span = pn.group * blk
    scale = -1.0 / (2.0 * pn.width)

    def tile(slot, xx, xv, lv, own):
        chi, clo = split(xv)
        nc = jnp.sum(xv * xv, axis=1, keepdims=True)
        l0 = lv[:, 0:1].astype(F32)
        proj = PROJ[slot]
        tot = TOT[slot:slot + 1, :]
        for j in range(n_col // pn.group):
            base = pl.multiple_of(xx * n_col * blk + j * span, span)
            rows = pl.ds(base, span)
            hi, lo, lb = RHI[rows, :], RLO[rows, :], RLB[rows, :]
            dots = nt(chi, hi) + nt(chi, lo) + nt(clo, hi)
            dist = jnp.maximum(nc + NR[:, rows] - 2.0 * dots, 0.0)
            kern = jnp.exp(dist * scale)
            if own:
                ids = lax.broadcasted_iota(jnp.int32, (blk, span), 1) + base
                mine = lax.broadcasted_iota(jnp.int32, (blk, span), 0) + me * blk
                kern = jnp.where(ids == mine, 0.0, kern)
            kh, kl = split(kern)
            proj = proj + nn(kh, lb) + nn(kl, lb)
            t = jnp.sum(kern, axis=0, keepdims=True)
            for g in range(pn.group):
                tot = tot + t[:, g * blk:(g + 1) * blk]
            if not own:
                ROWP[:, rows] += jnp.sum(kern * l0, axis=0, keepdims=True)
        PROJ[slot] = proj
        TOT[slot:slot + 1, :] = tot

    def line_tiles(hop, chunks, arrive):
        for b in routes:
            if hop <= routes[b][1]:
                at = b + routes[b][0] * hop

                @pl.when(z == at)
                def _():
                    if arrive and hop == routes[b][1]:
                        for ch in range(CHUNKS):
                            z_arrive(b, ch, at)
                    for xx in chunks:
                        tile(b, xx, CX[b], CL[b], False)

    def own_tile(xx):
        tile(nz, xx, x_ref[...], l_ref[...], True)

    prep(me, x_ref[...], l_ref[...])
    ROWP[...] = jnp.zeros_like(ROWP)
    PROJ[...] = jnp.zeros_like(PROJ)
    TOT[...] = jnp.zeros_like(TOT)

    def partner(k, part):
        if nk > 1:
            lev_send(k, part, dev(z, x, y, other))

    z_round(1, 0)
    for d in range(1, nx):
        k = lev_of(xm(d), y, core)
        lev_wait(k, A)
        for e in range(1, ny):
            lev_send(k, A, dev(z, x, ym(e), core))
        partner(k, A)
    for d in range(1, ny):
        k = lev_of(x, ym(d), core)
        lev_wait(k, B)
        for e in range(1, nx):
            lev_send(k, B, dev(z, xm(e), y, core))
        partner(k, B)
    z_round(1, 1)
    z_round(2, 0)
    z_round(1, 2)
    z_round(2, 1)
    z_round(1, 3)
    for d in range(1, ny):
        k = lev_of(x, ym(d), core)
        lev_wait(k, A)
        partner(k, A)
    for d in range(1, nx):
        k = lev_of(xm(d), y, core)
        lev_wait(k, B)
        partner(k, B)
    z_round(2, 2)

    def other_core(xx, ys):
        if nk > 1:
            for e in ys:
                for part in (A, B):
                    lev_wait(lev_of(xx, ym(e), other), part)

    other_core(x, range(ny))
    prep_chunk(x, 1)
    own_tile(x)
    z_round(2, 3)
    line_tiles(1, [x], True)
    for d in range(1, nx):
        for e in range(1, ny):
            k = lev_of(xm(d), ym(e), core)
            for part in (A, B):
                lev_wait(k, part)
                partner(k, part)
    far = [xm(d) for d in range(1, nx)]
    for xx in far:
        other_core(xx, range(ny))
        prep_chunk(xx, 0)
        own_tile(xx)
    line_tiles(1, far, False)
    for hop in range(2, nz):
        line_tiles(hop, [x] + far, True)

    quad = jnp.zeros((1, pn.perms), F32)
    tot = jnp.zeros((1, blk), F32)
    for b in list(routes) + [nz]:
        w = 1.0 if b == nz else 2.0
        lv = l_ref[...] if b == nz else CL[b]
        QUAD[b:b + 1, :] = jnp.zeros((1, pn.perms), F32)
        COLP[b:b + 1, :] = jnp.zeros((1, blk), F32)
        reach = [nz - 1] if b == nz else [b + routes[b][0] * h for h in range(1, routes[b][1] + 1)]

        @pl.when((z >= (0 if b == nz else min(reach))) & (z <= max(reach)))
        def _():
            QUAD[b:b + 1, :] = w * jnp.sum(lv.astype(F32) * PROJ[b], axis=0, keepdims=True)
            COLP[b:b + 1, :] = to_row(PROJ[b][:, 0:1])
        quad = quad + QUAD[b:b + 1, :]
        tot = tot + w * TOT[b:b + 1, :]
    own_proof = COLP[nz:nz + 1, :]

    qr = pn.perms // 128
    if direct:
        def head(ref, i):
            for j in range(qr):
                ref[i, j:j + 1, :] = quad[:, j * 128:(j + 1) * 128]
            ref[i, qr:qr + 1, :] = tot

        index = z * n_lev + me
        none = jnp.zeros((1, 128), F32)
        for k in range(n_lev):
            head(S1, k)
            S1[k, qr + 1:qr + 2, :] = ROWP[:, k * blk:(k + 1) * blk]
        for b in range(nz):
            head(S2, b)
            S2[b, qr + 1:qr + 2, :] = COLP[b:b + 1, :] if b in routes else none
        head(S2, nz)
        S2[nz, qr + 1:qr + 2, :] = none
        if nz > 1:
            pl.semaphore_wait(here, nz - 1)

        def x_copy(dz, d, slot):
            b, k = (z + dz) % nz, (me + d) % n_lev
            src = S1.at[k] if dz == 0 else (S2.at[b] if d == 0 else S2.at[nz])
            return pltpu.make_async_remote_copy(
                src_ref=src, dst_ref=R1.at[slot], send_sem=s1_send.at[dz * n_lev + d], recv_sem=s1_recv.at[slot],
                device_id=(b * nx + k // n_col, k % n_col), device_id_type=MESH)

        pairs = [(dz, d) for dz in reversed(range(nz)) for d in range(n_lev) if dz + d > 0]
        for dz, d in pairs:
            x_copy(dz, d, index).start()
        R1[index] = S1[me]
        for dz, d in pairs:
            x_copy(dz, d, ((z + dz) % nz) * n_lev + (me + d) % n_lev).wait_recv()
        done = R1[0]
        for i in range(1, n_dev):
            done = done + R1[i]
        proof = done[qr + 1:qr + 2, :] + own_proof
    else:
        for k in range(n_lev):
            for i in range(qr):
                S1[k, i:i + 1, :] = quad[:, i * 128:(i + 1) * 128]
            S1[k, qr:qr + 1, :] = tot
            S1[k, qr + 1:qr + 2, :] = ROWP[:, k * blk:(k + 1) * blk]

        def s1_copy(d):
            k = (me + d) % n_lev
            return pltpu.make_async_remote_copy(
                src_ref=S1.at[k], dst_ref=R1.at[me], send_sem=s1_send.at[k], recv_sem=s1_recv.at[me],
                device_id=lev_dev(k), device_id_type=MESH)

        def s1_in(d):
            k = (me + d) % n_lev
            return pltpu.make_async_remote_copy(
                src_ref=S1.at[k], dst_ref=R1.at[k], send_sem=s1_send.at[k], recv_sem=s1_recv.at[k],
                device_id=lev_dev(k), device_id_type=MESH)

        for d in range(1, n_lev):
            s1_copy(d).start()
        acc = S1[me]
        for d in range(1, n_lev):
            s1_in(d).wait_recv()
            acc = acc + R1[(me + d) % n_lev]
        for b in range(nz):
            S2[b, :, :] = acc
            S2[b, qr + 1:qr + 2, :] = COLP[b:b + 1, :] if b in routes else jnp.zeros((1, 128), F32)

        def s2_copy(d):
            b = (z + d) % nz
            return pltpu.make_async_remote_copy(
                src_ref=S2.at[b], dst_ref=R2.at[z], send_sem=s2_send.at[b], recv_sem=s2_recv.at[z],
                device_id=dev(b, x, y, core), device_id_type=MESH)

        def s2_in(d):
            b = (z + d) % nz
            return pltpu.make_async_remote_copy(
                src_ref=S2.at[b], dst_ref=R2.at[b], send_sem=s2_send.at[b], recv_sem=s2_recv.at[b],
                device_id=dev(b, x, y, core), device_id_type=MESH)

        for d in range(1, nz):
            s2_copy(d).start()
        for d in range(1, nz):
            s2_in(d).wait_recv()
        tops = []
        extra = jnp.zeros((1, 128), F32)
        for b in range(nz):
            mine = z == b
            tops.append(jnp.where(mine, acc, R2[b]))
            extra = extra + jnp.where(mine, 0.0, R2[b, qr + 1:qr + 2, :])
        done = functools.reduce(lambda u, v: u + v, tops)
        proof = acc[qr + 1:qr + 2, :] + own_proof + extra
    total = jnp.sum(done[qr:qr + 1, :], axis=1, keepdims=True)
    hf = pn.rows / 2.0
    den = 2.0 * hf * (hf - 1.0)
    stat = total / den + ((2.0 * hf - 1.0) / den) * done[0:qr, :]
    stat_ref[...] = stat
    proof_ref[...] = proof / math.sqrt(pn.rows)
    sg = 1.0 / (1.0 + jnp.exp(-4.0 * (stat - stat[0:1, 0:1])))
    first = (lax.broadcasted_iota(jnp.int32, stat.shape, 0) + lax.broadcasted_iota(jnp.int32, stat.shape, 1)) == 0
    sg = jnp.where(first, 0.0, sg)
    p = jnp.sum(jnp.sum(sg, axis=0, keepdims=True), axis=1, keepdims=True) / (pn.perms - 1)
    p_ref[...] = p

    for c in pending:
        c.wait_send()
    for b, ch, at, own, sems in z_pending:
        @pl.when(z == at)
        def _():
            for c in z_copy(b, ch, dev(at + routes[b][0], x, y, core), own, sems):
                c.wait_send()
    if direct:
        for dz, d in pairs:
            x_copy(dz, d, index).wait_send()
    else:
        for d in range(1, n_lev):
            s1_copy(d).wait_send()
        for d in range(1, nz):
            s2_copy(d).wait_send()
    assert counter[0] == n_send


def send_count(pn):
    nx, ny, nk, nz = pn.nx, pn.ny, pn.nk, pn.nz
    own = 2 * (nx - 1) + 2 * (ny - 1) + (2 if nk > 1 else 0)
    fwd = 2 * (nx - 1) * (ny - 1)
    core = 2 * (nx * ny - 1) if nk > 1 else 0
    line = sum(h for _, h in ROUTES[nz].values()) * CHUNKS
    return 2 * (own + fwd + core + line)


def line_kernel(x_hbm, l_hbm, out_ref, x_ref, l_ref, GX, GL, CX, CL, CC, HI, LO, LB, SH, SL, NR, NC, L0, OWN0,
                ROWP, PROJ, TOT, S1, R1, in_sem, xy_send, xy_recv, z_send, z_recv, m_send, m_recv, line, here):
    blk, width = x_ref.shape
    perms = l_ref.shape[1]
    nx, ny, nk, nz, n_lev = 2, 2, 2, 4, 8
    row, col = lax.axis_index("row"), lax.axis_index("col")
    z, x = row // nx, row % nx
    y, core = col // nk, col % nk
    qr = perms // 128
    A, B = 0, 1

    def dev(zz, xx, yy, kk):
        return (zz * nx + xx, yy * nk + kk)

    def signal(sem, to):
        pl.semaphore_signal(sem, inc=1, device_id=to, device_id_type=MESH)

    def remote(src, dst, ss, rs, to):
        return pltpu.make_async_remote_copy(src_ref=src, dst_ref=dst, send_sem=ss, recv_sem=rs, device_id=to,
                                            device_id_type=MESH)

    here_dev = (row, col)
    x_dev, y_dev, k_dev = dev(z, 1 - x, y, core), dev(z, x, 1 - y, core), dev(z, x, y, 1 - core)
    place = [(xx, yy, kk) for xx, yy, kk in ((x, y, core), (x, y, 1 - core), (1 - x, y, core), (x, 1 - y, core),
             (1 - x, y, 1 - core), (x, 1 - y, 1 - core), (1 - x, 1 - y, core), (1 - x, 1 - y, 1 - core))]

    loads = [pltpu.make_async_copy(x_hbm, x_ref, in_sem.at[0]), pltpu.make_async_copy(l_hbm, l_ref, in_sem.at[1])]
    for c in loads:
        c.start()
    barrier = pltpu.get_barrier_semaphore()
    for to in (x_dev, y_dev, k_dev):
        signal(barrier, to)

    @pl.when(z > 0)
    def _():
        signal(barrier, dev(z - 1, x, y, core))

    @pl.when(z < nz - 1)
    def _():
        signal(barrier, dev(z + 1, x, y, core))

    ROWP[...] = jnp.zeros_like(ROWP)
    PROJ[...] = jnp.zeros_like(PROJ)
    TOT[...] = jnp.zeros_like(TOT)
    for c in reversed(loads):
        c.wait()
    OWN0[...] = to_row(l_ref[:, 0:1].astype(F32)).astype(jnp.int32)
    pl.semaphore_wait(barrier, 3 + jnp.where(z > 0, 1, 0) + jnp.where(z < nz - 1, 1, 0))

    half = blk // 2

    def xy_copy(src, dst, part, i, to):
        r = pl.ds(part * half, half)
        mine, buf = ((x_ref, GX), (l_ref, GL))[i]
        s = mine.at[r] if src == 0 else buf.at[src, r]
        n = part * 2 + i
        return remote(s, buf.at[dst, r], xy_send.at[dst, n], xy_recv.at[dst, n], to)

    sent = []
    X, L = 0, 1

    def xy_start(src, dst, part, to, kinds=(X, L)):
        for i in kinds:
            c = xy_copy(src, dst, part, i, to)
            c.start()
            sent.append(c)

    def xy_wait(at, parts=(A, B), kinds=(X, L)):
        for part in parts:
            for i in kinds:
                xy_copy(at, at, part, i, here_dev).wait_recv()

    piece = blk // 4
    SAM, LAB = [0, 1, 2, 3], [5, 6, 7, 8]

    def z_copy(b, p, own, to):
        if p == 4:
            src, dst = (OWN0 if own else CC.at[b]), CC.at[b]
        else:
            r = pl.ds((p if p < 4 else p - 5) * piece, piece)
            mine, buf = (x_ref, CX) if p < 4 else (l_ref, CL)
            src, dst = (mine.at[r] if own else buf.at[b, r]), buf.at[b, r]
        return remote(src, dst, z_send.at[b, p], z_recv.at[b, p], to)

    def z_start(b, ps, own, step):
        for p in ps:
            z_copy(b, p, own, dev(z + step, x, y, core)).start()

    def z_wait(b, ps):
        for p in ps:
            z_copy(b, p, False, here_dev).wait_recv()

    def z_pass(b, ps, step):
        for p in ps:
            z_wait(b, [p])
            z_start(b, [p], False, step)

    def at_z(*levels):
        cond = z == levels[0]
        for v in levels[1:]:
            cond = cond | (z == v)
        return pl.when(cond)

    @at_z(0)
    def _():
        z_start(0, SAM + [4] + LAB, True, 1)

    @at_z(2)
    def _():
        z_start(2, SAM + [4], True, -1)
        signal(line, dev(1, x, y, core))

    @at_z(3)
    def _():
        z_start(3, SAM + [4] + LAB, True, -1)

    @at_z(1)
    def _():
        signal(line, dev(2, x, y, core))

    xy_start(0, 2, A, x_dev)
    xy_start(0, 3, B, y_dev)
    xy_start(0, 2, B, x_dev)
    xy_start(0, 3, A, y_dev)
    xy_start(0, 1, A, k_dev)
    xy_start(0, 1, B, k_dev)

    scale = -1.0 / (2.0 * width)
    span = nk * blk

    order = {0: [], 1: [0, 2, 3], 2: [3, 0], 3: [0]}

    def norms(v):
        return jnp.sum(v * v, axis=1, keepdims=True)

    def prep(at, v, lv):
        hi, lo = split(v)
        n = norms(v)
        rows = slice(at * blk, (at + 1) * blk)
        HI[rows, :] = hi
        LO[rows, :] = lo
        LB[rows, :] = lv.astype(F32).astype(BF16)
        NR[:, rows] = to_row(n)
        if at == 0:
            SH[rows, :] = hi
            SL[rows, :] = lo
            NC[rows, :] = n

    def prep_at(at):
        prep(at, GX[at], GL[at])

    def prep_line(b, j):
        hi, lo = split(CX[b])
        rows = slice(j * blk, (j + 1) * blk)
        SH[rows, :] = hi
        SL[rows, :] = lo
        NC[rows, :] = norms(CX[b])
        L0[rows, :] = jnp.transpose(jnp.broadcast_to(CC[b], (blk, blk)))[:, 0:1].astype(F32)

    def work(j0, j1, *groups):
        mine = slice(j0 * blk, j1 * blk)
        n = (j1 - j0) * blk
        tiles = []
        for g in groups:
            rows = slice(g * span, (g + 1) * span)
            hi = SH[mine, :]
            d = nt(jnp.concatenate([hi, SL[mine, :]], axis=0), HI[rows, :])
            tiles.append((g, rows, d[:n] + d[n:] + nt(hi, LO[rows, :])))
        for g, rows, dots in tiles:
            dist = jnp.maximum(NC[mine, :] + NR[:, rows] - 2.0 * dots, 0.0)
            kern = jnp.exp(dist * scale)
            if j0 == 0:
                top = kern[:blk]
                if g == 0:
                    gap = lax.broadcasted_iota(jnp.int32, top.shape, 1) - lax.broadcasted_iota(jnp.int32, top.shape, 0)
                    top = jnp.where(gap == 0, 0.0, top)
                    kern = top if n == blk else jnp.concatenate([top, kern[blk:]], axis=0)
                t = jnp.sum(top, axis=0, keepdims=True)
            else:
                t = jnp.zeros((1, span), F32)
            kh, kl = split(kern)
            p = nn(jnp.concatenate([kh, kl], axis=0), LB[rows, :])
            PROJ[mine, :] += p[:n] + p[n:]
            rest = kern[blk:] if j0 == 0 else kern
            if rest.shape[0]:
                t = t + 2.0 * jnp.sum(rest, axis=0, keepdims=True)
                line_rows = slice(max(j0, 1) * blk, j1 * blk)
                ROWP[:, rows] += jnp.sum(rest * L0[line_rows, :], axis=0, keepdims=True)
            TOT[...] += t[:, :blk] + t[:, blk:]

    prep(0, x_ref[...], l_ref[...])
    xy_wait(1)
    prep_at(1)

    @at_z(0, 3)
    def _():
        work(0, 1, 0)

    @at_z(1)
    def _():
        z_pass(0, [0, 1], 1)
        pl.semaphore_wait(line, 1)
        signal(line, dev(0, x, y, core))
        z_pass(0, [2], 1)

    @at_z(2)
    def _():
        z_pass(3, [0, 1], -1)
        pl.semaphore_wait(line, 1)
        signal(line, dev(3, x, y, core))
        z_pass(3, [2], -1)

    xy_wait(2, (A,))
    xy_start(2, 6, A, y_dev)
    xy_start(2, 4, A, k_dev)
    xy_wait(3, (B,))
    xy_start(3, 6, B, x_dev)
    xy_start(3, 5, B, k_dev)

    @at_z(1)
    def _():
        z_pass(0, [3, 4], 1)
        prep_line(0, 1)
        z_wait(2, SAM + [4])
        prep_line(2, 2)
        work(0, 3, 0)
        z_pass(0, LAB, 1)

    @at_z(2)
    def _():
        z_pass(3, [3, 4], -1)
        z_start(2, LAB, True, -1)
        prep_line(3, 1)
        z_pass(0, [0], 1)
        work(0, 2, 0)
        z_pass(0, [1], 1)
        z_pass(3, LAB[:3], -1)
        z_pass(0, [2], 1)
        z_pass(3, LAB[3:], -1)

    xy_wait(2, (B,))
    xy_start(2, 4, B, k_dev)
    xy_wait(3, (A,))
    xy_start(3, 5, A, k_dev)

    @at_z(0, 3)
    def _():
        pl.semaphore_wait(line, 1)

    signal(here.at[0], k_dev)
    prep_at(2)
    prep_at(3)

    @at_z(0, 3)
    def _():
        work(0, 1, 1)

    @at_z(1)
    def _():
        work(0, 3, 1)

    @at_z(2)
    def _():
        work(0, 2, 1)
        z_pass(0, [3, 4], 1)
        prep_line(0, 2)

    xy_wait(4)
    xy_wait(5)
    pl.semaphore_wait(here.at[0], 1)
    signal(here.at[1], x_dev)
    prep_at(4)
    prep_at(5)

    @at_z(0, 3)
    def _():
        work(0, 1, 2)

    @at_z(1)
    def _():
        work(0, 3, 2)

    @at_z(2)
    def _():
        work(0, 2, 2)
        z_pass(0, LAB[:2], 1)

    for part in (A, B):
        xy_wait(6, (part,), (X,))
        xy_start(6, 7, part, k_dev, (X,))
    pl.semaphore_wait(here.at[1], 1)
    signal(here.at[2], y_dev)

    @at_z(1)
    def _():
        z_wait(3, SAM + [4])
        prep_line(3, 3)
        work(3, 4, 0, 1, 2)

    for part in (A, B):
        xy_wait(6, (part,), (L,))
        xy_start(6, 7, part, k_dev, (L,))

    @at_z(2)
    def _():
        z_pass(0, LAB[2:], 1)
        work(2, 3, 0, 1, 2)

    @at_z(3)
    def _():
        z_wait(0, SAM + [4])
        prep_line(0, 1)
        work(1, 2, 0, 1, 2)

    prep_at(6)
    xy_wait(7)
    prep_at(7)
    for level in range(nz):
        @at_z(level)
        def _():
            work(0, 1 + len(order[level]), 3)

    def proj(j):
        return PROJ[j * blk:(j + 1) * blk, :]

    none = jnp.zeros((1, 128), F32)
    own_proof = to_row(proj(0)[:, 0:1])
    tot = TOT[...]
    for i in range(n_lev):
        S1[i, qr:qr + 1, :] = tot
        S1[i, qr + 1:qr + 2, :] = ROWP[:, i * blk:(i + 1) * blk]
    for b in range(nz + 1):
        S1[n_lev + b, qr:qr + 1, :] = tot
        S1[n_lev + b, qr + 1:qr + 2, :] = none
    for level in range(1, nz):
        @at_z(level)
        def _():
            for j, b in enumerate(order[level]):
                S1[n_lev + b, qr + 1:qr + 2, :] = to_row(proj(j + 1)[:, 0:1])

    def add(w, j, lv):
        q = w * jnp.sum(lv.astype(F32) * proj(j), axis=0, keepdims=True)
        for i in range(qr):
            S1[n_lev + nz, i:i + 1, :] += q[:, i * 128:(i + 1) * 128]

    S1[n_lev + nz, 0:qr, :] = jnp.zeros((qr, 128), F32)
    add(1.0, 0, l_ref[...])

    @at_z(3)
    def _():
        z_wait(0, LAB)

    @at_z(1, 3)
    def _():
        add(2.0, 1, CL[0])

    @at_z(2)
    def _():
        add(2.0, 1, CL[3])
        add(2.0, 2, CL[0])

    @at_z(1)
    def _():
        z_wait(2, LAB)
        add(2.0, 2, CL[2])
        z_wait(3, LAB)
        add(2.0, 3, CL[3])

    q = S1[n_lev + nz, 0:qr, :]
    for i in range(n_lev):
        S1[i, 0:qr, :] = q
    for b in range(nz):
        S1[n_lev + b, 0:qr, :] = q
    index = z * n_lev + x * 4 + col
    pl.semaphore_wait(here.at[2], 1)

    def m_copy(t, incoming):
        tz, tx, ty, tk = t // n_lev, t // 4 % nx, t // nk % ny, t % nk
        dx, dy, dk = jnp.where(tx == x, 0, 1), jnp.where(ty == y, 0, 1), jnp.where(tk == core, 0, 1)
        i = jnp.where(dk == 0, 2 * dx + 3 * dy + dx * dy, jnp.where(dx + dy == 0, 1, 3 + dx + 2 * dy + dx * dy))
        n = jnp.where(tz == z, i, n_lev + jnp.where(i == 0, tz, nz))
        return remote(S1.at[n], R1.at[t if incoming else index], m_send.at[t], m_recv.at[t if incoming else index],
                      dev(tz, tx, ty, tk))

    def others(act):
        for t in range(nz * n_lev):
            @pl.when(t != index)
            def _():
                act(t)

    others(lambda t: m_copy(t, False).start())
    R1[index] = S1[0]
    others(lambda t: m_copy(t, True).wait_recv())
    done = R1[0]
    for i in range(1, nz * n_lev):
        done = done + R1[i]
    out_ref[0:qr + 1, :] = done[0:qr + 1, :]
    out_ref[qr + 1:qr + 2, :] = done[qr + 1:qr + 2, :] + own_proof

    for c in sent:
        c.wait_send()
    for at, b in ((0, 0), (1, 0), (2, 0), (2, 2), (2, 3), (3, 3)):
        @at_z(at)
        def _():
            for p in SAM + [4] + LAB:
                z_copy(b, p, False, here_dev).wait_send()
    others(lambda t: m_copy(t, False).wait_send())


def finish(rows, perms, r_ref, stat_ref, proof_ref, p_ref):
    qr = perms // 128
    total = jnp.sum(r_ref[qr:qr + 1, :], axis=1, keepdims=True)
    hf = rows / 2.0
    den = 2.0 * hf * (hf - 1.0)
    stat = total / den + ((2.0 * hf - 1.0) / den) * r_ref[0:qr, :]
    stat_ref[...] = stat
    proof_ref[...] = r_ref[qr + 1:qr + 2, :] / math.sqrt(rows)
    sg = 1.0 / (1.0 + jnp.exp(-4.0 * (stat - stat[0:1, 0:1])))
    first = (lax.broadcasted_iota(jnp.int32, stat.shape, 0) + lax.broadcasted_iota(jnp.int32, stat.shape, 1)) == 0
    sg = jnp.where(first, 0.0, sg)
    p_ref[...] = jnp.sum(jnp.sum(sg, axis=0, keepdims=True), axis=1, keepdims=True) / (perms - 1)


def line_call(samples, labels):
    blk, width = samples.shape
    perms = labels.shape[1]
    qr = perms // 128
    nz, n_lev = 4, 8
    slots = nz * n_lev
    i32 = jnp.int32
    dma = pltpu.SemaphoreType.DMA
    vm = pl.BlockSpec(memory_space=pltpu.VMEM)
    hbm = pl.BlockSpec(memory_space=pl.ANY)
    res = pl.pallas_call(
        line_kernel,
        out_shape=jax.ShapeDtypeStruct((qr + 2, 128), F32),
        in_specs=[hbm, hbm],
        out_specs=vm,
        scratch_shapes=[
            pltpu.VMEM((blk, width), F32),
            pltpu.VMEM((blk, perms), i32),
            pltpu.VMEM((n_lev, blk, width), F32),
            pltpu.VMEM((n_lev, blk, perms), i32),
            pltpu.VMEM((nz, blk, width), F32),
            pltpu.VMEM((nz, blk, perms), i32),
            pltpu.VMEM((nz, 1, blk), i32),
            pltpu.VMEM((n_lev * blk, width), BF16),
            pltpu.VMEM((n_lev * blk, width), BF16),
            pltpu.VMEM((n_lev * blk, perms), BF16),
            pltpu.VMEM((nz * blk, width), BF16),
            pltpu.VMEM((nz * blk, width), BF16),
            pltpu.VMEM((1, n_lev * blk), F32),
            pltpu.VMEM((nz * blk, 1), F32),
            pltpu.VMEM((nz * blk, 1), F32),
            pltpu.VMEM((1, blk), i32),
            pltpu.VMEM((1, n_lev * blk), F32),
            pltpu.VMEM((nz * blk, perms), F32),
            pltpu.VMEM((1, blk), F32),
            pltpu.VMEM((n_lev + nz + 1, qr + 2, 128), F32),
            pltpu.VMEM((slots, qr + 2, 128), F32),
            dma((2,)),
            dma((n_lev, 4)),
            dma((n_lev, 4)),
            dma((nz, 9)),
            dma((nz, 9)),
            dma((slots,)),
            dma((slots,)),
            pltpu.SemaphoreType.REGULAR,
            pltpu.SemaphoreType.REGULAR((3,)),
        ],
        compiler_params=pltpu.CompilerParams(
            collective_id=1, has_side_effects=True, vmem_limit_bytes=LIMIT
        ),
    )(samples, labels)
    return pl.pallas_call(
        functools.partial(finish, blk * slots, perms),
        out_shape=(
            jax.ShapeDtypeStruct((qr, 128), F32),
            jax.ShapeDtypeStruct((1, blk), F32),
            jax.ShapeDtypeStruct((1, 1), F32),
        ),
        in_specs=[vm],
        out_specs=(vm, vm, vm),
    )(res)


def solution(mesh):
    n_row, n_col = mesh.shape["row"], mesh.shape["col"]

    def shards(samples, labels):
        blk, width = samples.shape
        perms = labels.shape[1]
        pn = Plan(n_row, n_col, blk, width, perms)
        n_send = send_count(pn)
        n_lev, nz = pn.n_lev, pn.nz
        if (pn.nx, pn.ny, pn.nk, nz, blk) == (2, 2, 2, 4, 128):
            stat, proof, p = line_call(samples, labels)
            return stat.reshape(perms), proof.reshape(blk), p.reshape(())
        msg = perms // 128 + 2
        slots = n_row * n_col if pn.direct else n_lev
        vm = pl.BlockSpec(memory_space=pltpu.VMEM)
        hbm = pl.BlockSpec(memory_space=pl.ANY)
        dma = pltpu.SemaphoreType.DMA
        stat, proof, p = pl.pallas_call(
            functools.partial(kernel, pn, n_send),
            out_shape=(
                jax.ShapeDtypeStruct((perms // 128, 128), F32),
                jax.ShapeDtypeStruct((1, blk), F32),
                jax.ShapeDtypeStruct((1, 1), F32),
            ),
            in_specs=[hbm, hbm],
            out_specs=(vm, vm, vm),
            scratch_shapes=[
                pltpu.VMEM((blk, width), F32),
                pltpu.VMEM((blk, perms), jnp.int32),
                pltpu.VMEM((n_lev, blk, width), F32),
                pltpu.VMEM((n_lev, blk, perms), jnp.int32),
                pltpu.VMEM((nz, blk, width), F32),
                pltpu.VMEM((nz, blk, perms), jnp.int32),
                pltpu.VMEM((n_lev * blk, width), BF16),
                pltpu.VMEM((n_lev * blk, width), BF16),
                pltpu.VMEM((n_lev * blk, perms), BF16),
                pltpu.VMEM((1, n_lev * blk), F32),
                pltpu.VMEM((1, n_lev * blk), F32),
                pltpu.VMEM((nz + 1, blk, perms), F32),
                pltpu.VMEM((nz + 1, perms), F32),
                pltpu.VMEM((nz + 1, blk), F32),
                pltpu.VMEM((nz + 1, blk), F32),
                pltpu.VMEM((n_lev, msg, 128), F32),
                pltpu.VMEM((slots, msg, 128), F32),
                pltpu.VMEM((nz + 1, msg, 128), F32),
                pltpu.VMEM((nz, msg, 128), F32),
                dma((2,)),
                dma((n_send,)),
                dma((n_lev, 2 * PARTS)),
                dma((nz, 2 * CHUNKS)),
                dma((slots,)),
                dma((slots,)),
                dma((nz,)),
                dma((nz,)),
                pltpu.SemaphoreType.REGULAR,
            ],
            compiler_params=pltpu.CompilerParams(
                collective_id=0, has_side_effects=True, vmem_limit_bytes=60 * 1024 * 1024
            ),
        )(samples, labels)
        return stat.reshape(perms), proof.reshape(blk), p.reshape(())

    placed = (P(("row", "col"), None), P(("row", "col"), None))
    return jax.shard_map(
        shards, mesh=mesh, in_specs=placed, out_specs=(P(), P(("row", "col")), P()), check_vma=False
    )
```

```python
import functools
import math

import jax
import jax.numpy as jnp
from jax import lax
from jax.experimental import pallas as pl
from jax.experimental.pallas import tpu as pltpu
from jax.sharding import PartitionSpec as P

MESH = pl.DeviceIdType.MESH
F32 = jnp.float32
BF16 = jnp.bfloat16
CHUNKS = 4
PARTS = 2
LIMIT = 60 * 1024 * 1024

ROUTES = {1: {}, 2: {0: (1, 1)}, 4: {0: (1, 3), 2: (-1, 1), 3: (-1, 2)}}


def nt(a, b):
    return lax.dot_general(a, b, (((1,), (1,)), ((), ())), preferred_element_type=F32)


def nn(a, b):
    return lax.dot_general(a, b, (((1,), (0,)), ((), ())), preferred_element_type=F32)


def split(v):
    hi = v.astype(BF16)
    return hi, (v - hi.astype(F32)).astype(BF16)


def to_row(column):
    n = column.shape[0]
    return jnp.transpose(jnp.broadcast_to(column, (n, n)))[0:1, :]


class Plan:
    def __init__(self, n_row, n_col, blk, width, perms):
        self.nz = math.gcd(n_row, 4)
        self.nx = n_row // self.nz
        self.nk = math.gcd(n_col, 2)
        self.ny = n_col // self.nk
        self.n_col = n_col
        self.n_lev = self.nx * n_col
        self.blk, self.width, self.perms = blk, width, perms
        self.direct = n_row * n_col <= 32
        self.group = math.gcd(n_col, 4)
        self.rows = blk * n_row * n_col


def kernel(pn, n_send, x_hbm, l_hbm, stat_ref, proof_ref, p_ref, x_ref, l_ref, RX, RL, CX, CL, RHI, RLO, RLB, NR,
           ROWP, PROJ, QUAD, TOT, COLP, S1, R1, S2, R2, in_sem, send, lev_sem, z_sem, s1_send, s1_recv, s2_send, s2_recv, here):
    nx, ny, nz, nk, n_col, n_lev, blk = pn.nx, pn.ny, pn.nz, pn.nk, pn.n_col, pn.n_lev, pn.blk
    row, col = lax.axis_index("row"), lax.axis_index("col")
    z, x = row // nx, row % nx
    y, core = col // nk, col % nk
    me = x * n_col + col
    routes = ROUTES[nz]
    pending = []

    def lev_of(xx, yy, kk):
        return xx * n_col + yy * nk + kk

    def dev(zz, xx, yy, kk):
        return (zz * nx + xx, yy * nk + kk)

    def lev_dev(k):
        return (z * nx + k // n_col, k % n_col)

    loads = [pltpu.make_async_copy(x_hbm, x_ref, in_sem.at[0]), pltpu.make_async_copy(l_hbm, l_ref, in_sem.at[1])]
    for c in loads:
        c.start()
    barrier = pltpu.get_barrier_semaphore()
    for d in range(1, n_lev):
        pl.semaphore_signal(barrier, inc=1, device_id=lev_dev((me + d) % n_lev), device_id_type=MESH)
    for d in range(1, nz):
        pl.semaphore_signal(barrier, inc=1, device_id=dev((z + d) % nz, x, y, core), device_id_type=MESH)
    pl.semaphore_wait(barrier, n_lev - 1 + nz - 1)
    for c in loads:
        c.wait()

    n_dev = nz * n_lev
    direct = pn.direct
    if direct:
        for d in range(1, nz):
            pl.semaphore_signal(here, inc=1, device_id=dev((z + d) % nz, x, y, core), device_id_type=MESH)

    counter = [0]

    def new_sem():
        counter[0] += 1
        return send.at[counter[0] - 1]

    half = blk // PARTS
    piece = blk // CHUNKS

    def lev_copy(k, part, target, own, sem):
        r = pl.ds(part * half, half)
        out = []
        for i, (src, dst) in enumerate(((x_ref, RX), (l_ref, RL))):
            s = src.at[r] if own else dst.at[k, r]
            out.append(pltpu.make_async_remote_copy(
                src_ref=s, dst_ref=dst.at[k, r], send_sem=new_sem() if sem else send.at[0],
                recv_sem=lev_sem.at[k, part * 2 + i], device_id=target, device_id_type=MESH))
        return out

    def lev_send(k, part, target, own=False):
        for c in lev_copy(k, part, target, own, True):
            c.start()
            pending.append(c)

    def lev_wait(k, part):
        for c in lev_copy(k, part, (row, col), False, False):
            c.wait_recv()

    def z_copy(b, ch, target, own, sems):
        r = pl.ds(ch * piece, piece)
        out = []
        for i, (src, dst) in enumerate(((x_ref, CX), (l_ref, CL))):
            s = src.at[r] if own else dst.at[b, r]
            out.append(pltpu.make_async_remote_copy(
                src_ref=s, dst_ref=dst.at[b, r], send_sem=sems[i],
                recv_sem=z_sem.at[b, ch * 2 + i], device_id=target, device_id_type=MESH))
        return out

    z_pending = []

    def z_send(b, ch, at, own):
        sems = [new_sem(), new_sem()]
        to = at + routes[b][0]

        @pl.when(z == at)
        def _():
            for c in z_copy(b, ch, dev(to, x, y, core), own, sems):
                c.start()
        z_pending.append((b, ch, at, own, sems))

    def z_arrive(b, ch, at):
        for c in z_copy(b, ch, (row, col), False, [send.at[0]] * 2):
            c.wait_recv()

    def z_round(hop, ch):
        for b in routes:
            if hop < routes[b][1]:
                at = b + routes[b][0] * hop

                @pl.when(z == at)
                def _():
                    z_arrive(b, ch, at)
                z_send(b, ch, at, False)

    def xm(d):
        return (x + d) % nx

    def ym(d):
        return (y + d) % ny

    other = (core + 1) % nk
    A, B = 0, 1
    for ch in range(CHUNKS):
        for b in routes:
            z_send(b, ch, b, True)
    for d in range(1, nx):
        lev_send(me, A, dev(z, xm(d), y, core), True)
    for d in range(1, ny):
        lev_send(me, B, dev(z, x, ym(d), core), True)
    for d in range(1, nx):
        lev_send(me, B, dev(z, xm(d), y, core), True)
    for d in range(1, ny):
        lev_send(me, A, dev(z, x, ym(d), core), True)
    if nk > 1:
        for part in (A, B):
            lev_send(me, part, dev(z, x, y, other), True)

    def prep(k, xv, lv):
        rows = pl.ds(pl.multiple_of(k * blk, blk), blk)
        hi, lo = split(xv)
        RHI[rows, :] = hi
        RLO[rows, :] = lo
        RLB[rows, :] = lv.astype(F32).astype(BF16)
        NR[:, rows] = to_row(jnp.sum(xv * xv, axis=1, keepdims=True))

    def prep_chunk(xx, skip):
        def step(i, _):
            k = xx * n_col + (col + i) % n_col
            prep(k, RX[k], RL[k])
            return 0

        lax.fori_loop(skip, n_col, step, 0)

    span = pn.group * blk
    scale = -1.0 / (2.0 * pn.width)

    def tile(slot, xx, xv, lv, own):
        chi, clo = split(xv)
        nc = jnp.sum(xv * xv, axis=1, keepdims=True)
        l0 = lv[:, 0:1].astype(F32)
        proj = PROJ[slot]
        tot = TOT[slot:slot + 1, :]
        for j in range(n_col // pn.group):
            base = pl.multiple_of(xx * n_col * blk + j * span, span)
            rows = pl.ds(base, span)
            hi, lo, lb = RHI[rows, :], RLO[rows, :], RLB[rows, :]
            dots = nt(chi, hi) + nt(chi, lo) + nt(clo, hi)
            dist = jnp.maximum(nc + NR[:, rows] - 2.0 * dots, 0.0)
            kern = jnp.exp(dist * scale)
            if own:
                ids = lax.broadcasted_iota(jnp.int32, (blk, span), 1) + base
                mine = lax.broadcasted_iota(jnp.int32, (blk, span), 0) + me * blk
                kern = jnp.where(ids == mine, 0.0, kern)
            kh, kl = split(kern)
            proj = proj + nn(kh, lb) + nn(kl, lb)
            t = jnp.sum(kern, axis=0, keepdims=True)
            for g in range(pn.group):
                tot = tot + t[:, g * blk:(g + 1) * blk]
            if not own:
                ROWP[:, rows] += jnp.sum(kern * l0, axis=0, keepdims=True)
        PROJ[slot] = proj
        TOT[slot:slot + 1, :] = tot

    def line_tiles(hop, chunks, arrive):
        for b in routes:
            if hop <= routes[b][1]:
                at = b + routes[b][0] * hop

                @pl.when(z == at)
                def _():
                    if arrive and hop == routes[b][1]:
                        for ch in range(CHUNKS):
                            z_arrive(b, ch, at)
                    for xx in chunks:
                        tile(b, xx, CX[b], CL[b], False)

    def own_tile(xx):
        tile(nz, xx, x_ref[...], l_ref[...], True)

    prep(me, x_ref[...], l_ref[...])
    ROWP[...] = jnp.zeros_like(ROWP)
    PROJ[...] = jnp.zeros_like(PROJ)
    TOT[...] = jnp.zeros_like(TOT)

    def partner(k, part):
        if nk > 1:
            lev_send(k, part, dev(z, x, y, other))

    z_round(1, 0)
    for d in range(1, nx):
        k = lev_of(xm(d), y, core)
        lev_wait(k, A)
        for e in range(1, ny):
            lev_send(k, A, dev(z, x, ym(e), core))
        partner(k, A)
    for d in range(1, ny):
        k = lev_of(x, ym(d), core)
        lev_wait(k, B)
        for e in range(1, nx):
            lev_send(k, B, dev(z, xm(e), y, core))
        partner(k, B)
    z_round(1, 1)
    z_round(2, 0)
    z_round(1, 2)
    z_round(2, 1)
    z_round(1, 3)
    for d in range(1, ny):
        k = lev_of(x, ym(d), core)
        lev_wait(k, A)
        partner(k, A)
    for d in range(1, nx):
        k = lev_of(xm(d), y, core)
        lev_wait(k, B)
        partner(k, B)
    z_round(2, 2)

    def other_core(xx, ys):
        if nk > 1:
            for e in ys:
                for part in (A, B):
                    lev_wait(lev_of(xx, ym(e), other), part)

    other_core(x, range(ny))
    prep_chunk(x, 1)
    own_tile(x)
    z_round(2, 3)
    line_tiles(1, [x], True)
    for d in range(1, nx):
        for e in range(1, ny):
            k = lev_of(xm(d), ym(e), core)
            for part in (A, B):
                lev_wait(k, part)
                partner(k, part)
    far = [xm(d) for d in range(1, nx)]
    for xx in far:
        other_core(xx, range(ny))
        prep_chunk(xx, 0)
        own_tile(xx)
    line_tiles(1, far, False)
    for hop in range(2, nz):
        line_tiles(hop, [x] + far, True)

    quad = jnp.zeros((1, pn.perms), F32)
    tot = jnp.zeros((1, blk), F32)
    for b in list(routes) + [nz]:
        w = 1.0 if b == nz else 2.0
        lv = l_ref[...] if b == nz else CL[b]
        QUAD[b:b + 1, :] = jnp.zeros((1, pn.perms), F32)
        COLP[b:b + 1, :] = jnp.zeros((1, blk), F32)
        reach = [nz - 1] if b == nz else [b + routes[b][0] * h for h in range(1, routes[b][1] + 1)]

        @pl.when((z >= (0 if b == nz else min(reach))) & (z <= max(reach)))
        def _():
            QUAD[b:b + 1, :] = w * jnp.sum(lv.astype(F32) * PROJ[b], axis=0, keepdims=True)
            COLP[b:b + 1, :] = to_row(PROJ[b][:, 0:1])
        quad = quad + QUAD[b:b + 1, :]
        tot = tot + w * TOT[b:b + 1, :]
    own_proof = COLP[nz:nz + 1, :]

    qr = pn.perms // 128
    if direct:
        def head(ref, i):
            for j in range(qr):
                ref[i, j:j + 1, :] = quad[:, j * 128:(j + 1) * 128]
            ref[i, qr:qr + 1, :] = tot

        index = z * n_lev + me
        none = jnp.zeros((1, 128), F32)
        for k in range(n_lev):
            head(S1, k)
            S1[k, qr + 1:qr + 2, :] = ROWP[:, k * blk:(k + 1) * blk]
        for b in range(nz):
            head(S2, b)
            S2[b, qr + 1:qr + 2, :] = COLP[b:b + 1, :] if b in routes else none
        head(S2, nz)
        S2[nz, qr + 1:qr + 2, :] = none
        if nz > 1:
            pl.semaphore_wait(here, nz - 1)

        def x_copy(dz, d, slot):
            b, k = (z + dz) % nz, (me + d) % n_lev
            src = S1.at[k] if dz == 0 else (S2.at[b] if d == 0 else S2.at[nz])
            return pltpu.make_async_remote_copy(
                src_ref=src, dst_ref=R1.at[slot], send_sem=s1_send.at[dz * n_lev + d], recv_sem=s1_recv.at[slot],
                device_id=(b * nx + k // n_col, k % n_col), device_id_type=MESH)

        pairs = [(dz, d) for dz in reversed(range(nz)) for d in range(n_lev) if dz + d > 0]
        for dz, d in pairs:
            x_copy(dz, d, index).start()
        R1[index] = S1[me]
        for dz, d in pairs:
            x_copy(dz, d, ((z + dz) % nz) * n_lev + (me + d) % n_lev).wait_recv()
        done = R1[0]
        for i in range(1, n_dev):
            done = done + R1[i]
        proof = done[qr + 1:qr + 2, :] + own_proof
    else:
        for k in range(n_lev):
            for i in range(qr):
                S1[k, i:i + 1, :] = quad[:, i * 128:(i + 1) * 128]
            S1[k, qr:qr + 1, :] = tot
            S1[k, qr + 1:qr + 2, :] = ROWP[:, k * blk:(k + 1) * blk]

        def s1_copy(d):
            k = (me + d) % n_lev
            return pltpu.make_async_remote_copy(
                src_ref=S1.at[k], dst_ref=R1.at[me], send_sem=s1_send.at[k], recv_sem=s1_recv.at[me],
                device_id=lev_dev(k), device_id_type=MESH)

        def s1_in(d):
            k = (me + d) % n_lev
            return pltpu.make_async_remote_copy(
                src_ref=S1.at[k], dst_ref=R1.at[k], send_sem=s1_send.at[k], recv_sem=s1_recv.at[k],
                device_id=lev_dev(k), device_id_type=MESH)

        for d in range(1, n_lev):
            s1_copy(d).start()
        acc = S1[me]
        for d in range(1, n_lev):
            s1_in(d).wait_recv()
            acc = acc + R1[(me + d) % n_lev]
        for b in range(nz):
            S2[b, :, :] = acc
            S2[b, qr + 1:qr + 2, :] = COLP[b:b + 1, :] if b in routes else jnp.zeros((1, 128), F32)

        def s2_copy(d):
            b = (z + d) % nz
            return pltpu.make_async_remote_copy(
                src_ref=S2.at[b], dst_ref=R2.at[z], send_sem=s2_send.at[b], recv_sem=s2_recv.at[z],
                device_id=dev(b, x, y, core), device_id_type=MESH)

        def s2_in(d):
            b = (z + d) % nz
            return pltpu.make_async_remote_copy(
                src_ref=S2.at[b], dst_ref=R2.at[b], send_sem=s2_send.at[b], recv_sem=s2_recv.at[b],
                device_id=dev(b, x, y, core), device_id_type=MESH)

        for d in range(1, nz):
            s2_copy(d).start()
        for d in range(1, nz):
            s2_in(d).wait_recv()
        tops = []
        extra = jnp.zeros((1, 128), F32)
        for b in range(nz):
            mine = z == b
            tops.append(jnp.where(mine, acc, R2[b]))
            extra = extra + jnp.where(mine, 0.0, R2[b, qr + 1:qr + 2, :])
        done = functools.reduce(lambda u, v: u + v, tops)
        proof = acc[qr + 1:qr + 2, :] + own_proof + extra
    total = jnp.sum(done[qr:qr + 1, :], axis=1, keepdims=True)
    hf = pn.rows / 2.0
    den = 2.0 * hf * (hf - 1.0)
    stat = total / den + ((2.0 * hf - 1.0) / den) * done[0:qr, :]
    stat_ref[...] = stat
    proof_ref[...] = proof / math.sqrt(pn.rows)
    sg = 1.0 / (1.0 + jnp.exp(-4.0 * (stat - stat[0:1, 0:1])))
    first = (lax.broadcasted_iota(jnp.int32, stat.shape, 0) + lax.broadcasted_iota(jnp.int32, stat.shape, 1)) == 0
    sg = jnp.where(first, 0.0, sg)
    p = jnp.sum(jnp.sum(sg, axis=0, keepdims=True), axis=1, keepdims=True) / (pn.perms - 1)
    p_ref[...] = p

    for c in pending:
        c.wait_send()
    for b, ch, at, own, sems in z_pending:
        @pl.when(z == at)
        def _():
            for c in z_copy(b, ch, dev(at + routes[b][0], x, y, core), own, sems):
                c.wait_send()
    if direct:
        for dz, d in pairs:
            x_copy(dz, d, index).wait_send()
    else:
        for d in range(1, n_lev):
            s1_copy(d).wait_send()
        for d in range(1, nz):
            s2_copy(d).wait_send()
    assert counter[0] == n_send


def send_count(pn):
    nx, ny, nk, nz = pn.nx, pn.ny, pn.nk, pn.nz
    own = 2 * (nx - 1) + 2 * (ny - 1) + (2 if nk > 1 else 0)
    fwd = 2 * (nx - 1) * (ny - 1)
    core = 2 * (nx * ny - 1) if nk > 1 else 0
    line = sum(h for _, h in ROUTES[nz].values()) * CHUNKS
    return 2 * (own + fwd + core + line)


def line_kernel(x_hbm, l_hbm, out_ref, x_ref, l_ref, GX, GL, CX, CL, CC, HI, LO, LB, SH, SL, NR, NC, L0, OWN0,
                ROWP, PROJ, TOT, S1, R1, in_sem, xy_send, xy_recv, z_send, z_recv, m_send, m_recv, line, here):
    blk, width = x_ref.shape
    perms = l_ref.shape[1]
    nx, ny, nk, nz, n_lev = 2, 2, 2, 4, 8
    row, col = lax.axis_index("row"), lax.axis_index("col")
    z, x = row // nx, row % nx
    y, core = col // nk, col % nk
    qr = perms // 128
    A, B, ALL = 0, 1, 2

    def dev(zz, xx, yy, kk):
        return (zz * nx + xx, yy * nk + kk)

    def signal(sem, to):
        pl.semaphore_signal(sem, inc=1, device_id=to, device_id_type=MESH)

    def remote(src, dst, ss, rs, to):
        return pltpu.make_async_remote_copy(src_ref=src, dst_ref=dst, send_sem=ss, recv_sem=rs, device_id=to,
                                            device_id_type=MESH)

    here_dev = (row, col)
    x_dev, y_dev, k_dev = dev(z, 1 - x, y, core), dev(z, x, 1 - y, core), dev(z, x, y, 1 - core)
    place = [(xx, yy, kk) for xx, yy, kk in ((x, y, core), (x, y, 1 - core), (1 - x, y, core), (x, 1 - y, core),
             (1 - x, y, 1 - core), (x, 1 - y, 1 - core), (1 - x, 1 - y, core), (1 - x, 1 - y, 1 - core))]

    loads = [pltpu.make_async_copy(x_hbm, x_ref, in_sem.at[0]), pltpu.make_async_copy(l_hbm, l_ref, in_sem.at[1])]
    for c in loads:
        c.start()
    barrier = pltpu.get_barrier_semaphore()
    for to in (x_dev, y_dev, k_dev):
        signal(barrier, to)

    @pl.when(z > 0)
    def _():
        signal(barrier, dev(z - 1, x, y, core))

    @pl.when(z < nz - 1)
    def _():
        signal(barrier, dev(z + 1, x, y, core))

    ROWP[...] = jnp.zeros_like(ROWP)
    PROJ[...] = jnp.zeros_like(PROJ)
    TOT[...] = jnp.zeros_like(TOT)
    for c in reversed(loads):
        c.wait()
    OWN0[...] = to_row(l_ref[:, 0:1].astype(F32)).astype(jnp.int32)
    pl.semaphore_wait(barrier, 3 + jnp.where(z > 0, 1, 0) + jnp.where(z < nz - 1, 1, 0))

    half = blk // 2

    def xy_copy(src, dst, part, i, to):
        r = pl.ds(part * half, half) if part < 2 else pl.ds(0, blk)
        mine, buf = ((x_ref, GX), (l_ref, GL))[i]
        s = mine.at[r] if src == 0 else buf.at[src, r]
        n = part % 2 * 2 + i
        return remote(s, buf.at[dst, r], xy_send.at[dst, n], xy_recv.at[dst, n], to)

    sent = []
    X, L = 0, 1

    def xy_start(src, dst, part, to, kinds=(X, L)):
        for i in kinds:
            c = xy_copy(src, dst, part, i, to)
            c.start()
            sent.append(c)

    def xy_wait(at, parts=(A, B), kinds=(X, L)):
        for part in parts:
            for i in kinds:
                xy_copy(at, at, part, i, here_dev).wait_recv()

    piece = blk // 4
    SAM, LAB = [0, 1, 2, 3], [5, 6, 7, 8]

    EACH = {p: (p % 5, p % 5 + 1) for p in SAM + LAB}
    WHOLE = {3: (0, 4), 8: (0, 4)}
    CUTS = {0: EACH, 2: WHOLE, 3: {1: (0, 2), 3: (2, 4), 8: (0, 4)}}

    def held(b, ps):
        return [p for p in ps if p == 4 or p in CUTS[b]]

    def z_copy(b, p, own, to):
        if p == 4:
            src, dst = (OWN0 if own else CC.at[b]), CC.at[b]
        else:
            first, end = CUTS[b][p]
            r = pl.ds(first * piece, (end - first) * piece)
            mine, buf = (x_ref, CX) if p < 4 else (l_ref, CL)
            src, dst = (mine.at[r] if own else buf.at[b, r]), buf.at[b, r]
        return remote(src, dst, z_send.at[b, p], z_recv.at[b, p], to)

    def z_start(b, ps, own, step):
        for p in held(b, ps):
            z_copy(b, p, own, dev(z + step, x, y, core)).start()

    def z_wait(b, ps):
        for p in held(b, ps):
            z_copy(b, p, False, here_dev).wait_recv()

    def z_pass(b, ps, step):
        for p in held(b, ps):
            z_wait(b, [p])
            z_start(b, [p], False, step)

    def at_z(*levels):
        cond = z == levels[0]
        for v in levels[1:]:
            cond = cond | (z == v)
        return pl.when(cond)

    @at_z(0)
    def _():
        z_start(0, SAM + [4] + LAB, True, 1)

    @at_z(2)
    def _():
        z_start(2, SAM + [4], True, -1)
        signal(line, dev(1, x, y, core))

    @at_z(3)
    def _():
        z_start(3, SAM + [4] + LAB, True, -1)

    @at_z(1)
    def _():
        signal(line, dev(2, x, y, core))

    xy_start(0, 2, A, x_dev)
    xy_start(0, 3, B, y_dev)
    xy_start(0, 2, B, x_dev)
    xy_start(0, 3, A, y_dev)
    xy_start(0, 1, ALL, k_dev)

    scale = -1.0 / (2.0 * width)
    span = nk * blk

    order = {0: [], 1: [0, 2, 3], 2: [3, 0], 3: [0]}

    def norms(v):
        return jnp.sum(v * v, axis=1, keepdims=True)

    def prep(at, v, lv):
        hi, lo = split(v)
        n = norms(v)
        rows = slice(at * blk, (at + 1) * blk)
        HI[rows, :] = hi
        LO[rows, :] = lo
        LB[rows, :] = lv.astype(F32).astype(BF16)
        NR[:, rows] = to_row(n)
        if at == 0:
            SH[rows, :] = hi
            SL[rows, :] = lo
            NC[rows, :] = n

    def prep_at(at):
        prep(at, GX[at], GL[at])

    def prep_line(b, j):
        hi, lo = split(CX[b])
        rows = slice(j * blk, (j + 1) * blk)
        SH[rows, :] = hi
        SL[rows, :] = lo
        NC[rows, :] = norms(CX[b])
        L0[rows, :] = jnp.transpose(jnp.broadcast_to(CC[b], (blk, blk)))[:, 0:1].astype(F32)

    def work(j0, j1, *groups):
        mine = slice(j0 * blk, j1 * blk)
        n = (j1 - j0) * blk
        tiles = []
        for g in groups:
            rows = slice(g * span, (g + 1) * span)
            hi = SH[mine, :]
            d = nt(jnp.concatenate([hi, SL[mine, :]], axis=0), HI[rows, :])
            tiles.append((g, rows, d[:n] + d[n:] + nt(hi, LO[rows, :])))
        for g, rows, dots in tiles:
            dist = jnp.maximum(NC[mine, :] + NR[:, rows] - 2.0 * dots, 0.0)
            kern = jnp.exp(dist * scale)
            if j0 == 0:
                top = kern[:blk]
                if g == 0:
                    gap = lax.broadcasted_iota(jnp.int32, top.shape, 1) - lax.broadcasted_iota(jnp.int32, top.shape, 0)
                    top = jnp.where(gap == 0, 0.0, top)
                    kern = top if n == blk else jnp.concatenate([top, kern[blk:]], axis=0)
                t = jnp.sum(top, axis=0, keepdims=True)
            else:
                t = jnp.zeros((1, span), F32)
            kh, kl = split(kern)
            p = nn(jnp.concatenate([kh, kl], axis=0), LB[rows, :])
            PROJ[mine, :] += p[:n] + p[n:]
            rest = kern[blk:] if j0 == 0 else kern
            if rest.shape[0]:
                t = t + 2.0 * jnp.sum(rest, axis=0, keepdims=True)
                line_rows = slice(max(j0, 1) * blk, j1 * blk)
                ROWP[:, rows] += jnp.sum(rest * L0[line_rows, :], axis=0, keepdims=True)
            TOT[...] += t[:, :blk] + t[:, blk:]

    prep(0, x_ref[...], l_ref[...])
    xy_wait(1, (ALL,))
    prep_at(1)

    @at_z(0, 3)
    def _():
        work(0, 1, 0)

    @at_z(1)
    def _():
        z_pass(0, [0, 1], 1)
        pl.semaphore_wait(line, 1)
        signal(line, dev(0, x, y, core))
        z_pass(0, [2], 1)

    @at_z(2)
    def _():
        z_pass(3, [0, 1], -1)
        pl.semaphore_wait(line, 1)
        signal(line, dev(3, x, y, core))
        z_pass(3, [2], -1)

    xy_wait(2, (A,))
    xy_start(2, 6, A, y_dev)
    xy_start(2, 4, A, k_dev)
    xy_wait(3, (B,))
    xy_start(3, 6, B, x_dev)
    xy_start(3, 5, B, k_dev)

    @at_z(1)
    def _():
        z_pass(0, [3, 4], 1)
        prep_line(0, 1)
        z_wait(2, SAM + [4])
        prep_line(2, 2)
        work(0, 3, 0)
        z_pass(0, LAB, 1)

    @at_z(2)
    def _():
        z_pass(3, [3, 4], -1)
        z_start(2, LAB, True, -1)
        prep_line(3, 1)
        z_pass(0, [0], 1)
        work(0, 2, 0)
        z_pass(0, [1], 1)
        z_pass(3, LAB[:3], -1)
        z_pass(0, [2], 1)
        z_pass(3, LAB[3:], -1)

    xy_wait(2, (B,))
    xy_start(2, 4, B, k_dev)
    xy_wait(3, (A,))
    xy_start(3, 5, A, k_dev)

    @at_z(0, 3)
    def _():
        pl.semaphore_wait(line, 1)

    signal(here.at[0], k_dev)
    prep_at(2)
    prep_at(3)

    @at_z(0, 3)
    def _():
        work(0, 1, 1)

    @at_z(1)
    def _():
        work(0, 3, 1)

    @at_z(2)
    def _():
        work(0, 2, 1)
        z_pass(0, [3, 4], 1)
        prep_line(0, 2)

    xy_wait(4)
    xy_wait(5)
    pl.semaphore_wait(here.at[0], 1)
    signal(here.at[1], x_dev)
    prep_at(4)
    prep_at(5)

    @at_z(0, 3)
    def _():
        work(0, 1, 2)

    @at_z(1)
    def _():
        work(0, 3, 2)

    @at_z(2)
    def _():
        work(0, 2, 2)
        z_pass(0, LAB[:2], 1)

    xy_wait(6, (A, B), (X,))
    xy_start(6, 7, ALL, k_dev, (X,))
    pl.semaphore_wait(here.at[1], 1)
    signal(here.at[2], y_dev)

    @at_z(1)
    def _():
        z_wait(3, SAM + [4])
        prep_line(3, 3)
        work(3, 4, 0, 1, 2)

    xy_wait(6, (A, B), (L,))
    xy_start(6, 7, ALL, k_dev, (L,))

    @at_z(2)
    def _():
        z_pass(0, LAB[2:], 1)
        work(2, 3, 0, 1, 2)

    prep_at(6)

    @at_z(3)
    def _():
        z_wait(0, SAM + [4])
        prep_line(0, 1)
        work(1, 2, 0, 1, 2)

    xy_wait(7, (ALL,))
    prep_at(7)
    for level in range(nz):
        @at_z(level)
        def _():
            work(0, 1 + len(order[level]), 3)

    def proj(j):
        return PROJ[j * blk:(j + 1) * blk, :]

    none = jnp.zeros((1, 128), F32)
    own_proof = to_row(proj(0)[:, 0:1])
    tot = TOT[...]
    for i in range(n_lev):
        S1[i, qr:qr + 1, :] = tot
        S1[i, qr + 1:qr + 2, :] = ROWP[:, i * blk:(i + 1) * blk]
    for b in range(nz + 1):
        S1[n_lev + b, qr:qr + 1, :] = tot
        S1[n_lev + b, qr + 1:qr + 2, :] = none
    for level in range(1, nz):
        @at_z(level)
        def _():
            for j, b in enumerate(order[level]):
                S1[n_lev + b, qr + 1:qr + 2, :] = to_row(proj(j + 1)[:, 0:1])

    def add(w, j, lv):
        q = w * jnp.sum(lv.astype(F32) * proj(j), axis=0, keepdims=True)
        for i in range(qr):
            S1[n_lev + nz, i:i + 1, :] += q[:, i * 128:(i + 1) * 128]

    S1[n_lev + nz, 0:qr, :] = jnp.zeros((qr, 128), F32)
    add(1.0, 0, l_ref[...])

    @at_z(3)
    def _():
        z_wait(0, LAB)

    @at_z(1, 3)
    def _():
        add(2.0, 1, CL[0])

    @at_z(2)
    def _():
        add(2.0, 1, CL[3])
        add(2.0, 2, CL[0])

    @at_z(1)
    def _():
        z_wait(2, LAB)
        add(2.0, 2, CL[2])
        z_wait(3, LAB)
        add(2.0, 3, CL[3])

    q = S1[n_lev + nz, 0:qr, :]
    for i in range(n_lev):
        S1[i, 0:qr, :] = q
    for b in range(nz):
        S1[n_lev + b, 0:qr, :] = q
    index = z * n_lev + x * 4 + col
    pl.semaphore_wait(here.at[2], 1)

    def m_copy(t, incoming):
        tz, tx, ty, tk = t // n_lev, t // 4 % nx, t // nk % ny, t % nk
        dx, dy, dk = jnp.where(tx == x, 0, 1), jnp.where(ty == y, 0, 1), jnp.where(tk == core, 0, 1)
        i = jnp.where(dk == 0, 2 * dx + 3 * dy + dx * dy, jnp.where(dx + dy == 0, 1, 3 + dx + 2 * dy + dx * dy))
        n = jnp.where(tz == z, i, n_lev + jnp.where(i == 0, tz, nz))
        return remote(S1.at[n], R1.at[t if incoming else index], m_send.at[t], m_recv.at[t if incoming else index],
                      dev(tz, tx, ty, tk))

    def others(act):
        for t in range(nz * n_lev):
            @pl.when(t != index)
            def _():
                act(t)

    others(lambda t: m_copy(t, False).start())
    R1[index] = S1[0]

    for c in sent:
        c.wait_send()
    for at, b in ((0, 0), (1, 0), (2, 0), (2, 2), (2, 3), (3, 3)):
        @at_z(at)
        def _():
            for p in held(b, SAM + [4] + LAB):
                z_copy(b, p, False, here_dev).wait_send()

    others(lambda t: m_copy(t, False).wait_send())
    done = jnp.zeros((qr + 2, 128), F32)
    for t in range(nz * n_lev):
        @pl.when(t != index)
        def _():
            m_copy(t, True).wait_recv()
        done = done + R1[t]
    out_ref[0:qr + 1, :] = done[0:qr + 1, :]
    out_ref[qr + 1:qr + 2, :] = done[qr + 1:qr + 2, :] + own_proof


def finish(rows, perms, r_ref, stat_ref, proof_ref, p_ref):
    qr = perms // 128
    total = jnp.sum(r_ref[qr:qr + 1, :], axis=1, keepdims=True)
    hf = rows / 2.0
    den = 2.0 * hf * (hf - 1.0)
    stat = total / den + ((2.0 * hf - 1.0) / den) * r_ref[0:qr, :]
    stat_ref[...] = stat
    proof_ref[...] = r_ref[qr + 1:qr + 2, :] / math.sqrt(rows)
    sg = 1.0 / (1.0 + jnp.exp(-4.0 * (stat - stat[0:1, 0:1])))
    first = (lax.broadcasted_iota(jnp.int32, stat.shape, 0) + lax.broadcasted_iota(jnp.int32, stat.shape, 1)) == 0
    sg = jnp.where(first, 0.0, sg)
    p_ref[...] = jnp.sum(jnp.sum(sg, axis=0, keepdims=True), axis=1, keepdims=True) / (perms - 1)


def line_call(samples, labels):
    blk, width = samples.shape
    perms = labels.shape[1]
    qr = perms // 128
    nz, n_lev = 4, 8
    slots = nz * n_lev
    i32 = jnp.int32
    dma = pltpu.SemaphoreType.DMA
    vm = pl.BlockSpec(memory_space=pltpu.VMEM)
    hbm = pl.BlockSpec(memory_space=pl.ANY)
    res = pl.pallas_call(
        line_kernel,
        out_shape=jax.ShapeDtypeStruct((qr + 2, 128), F32),
        in_specs=[hbm, hbm],
        out_specs=vm,
        scratch_shapes=[
            pltpu.VMEM((blk, width), F32),
            pltpu.VMEM((blk, perms), i32),
            pltpu.VMEM((n_lev, blk, width), F32),
            pltpu.VMEM((n_lev, blk, perms), i32),
            pltpu.VMEM((nz, blk, width), F32),
            pltpu.VMEM((nz, blk, perms), i32),
            pltpu.VMEM((nz, 1, blk), i32),
            pltpu.VMEM((n_lev * blk, width), BF16),
            pltpu.VMEM((n_lev * blk, width), BF16),
            pltpu.VMEM((n_lev * blk, perms), BF16),
            pltpu.VMEM((nz * blk, width), BF16),
            pltpu.VMEM((nz * blk, width), BF16),
            pltpu.VMEM((1, n_lev * blk), F32),
            pltpu.VMEM((nz * blk, 1), F32),
            pltpu.VMEM((nz * blk, 1), F32),
            pltpu.VMEM((1, blk), i32),
            pltpu.VMEM((1, n_lev * blk), F32),
            pltpu.VMEM((nz * blk, perms), F32),
            pltpu.VMEM((1, blk), F32),
            pltpu.VMEM((n_lev + nz + 1, qr + 2, 128), F32),
            pltpu.VMEM((slots, qr + 2, 128), F32),
            dma((2,)),
            dma((n_lev, 4)),
            dma((n_lev, 4)),
            dma((nz, 9)),
            dma((nz, 9)),
            dma((slots,)),
            dma((slots,)),
            pltpu.SemaphoreType.REGULAR,
            pltpu.SemaphoreType.REGULAR((3,)),
        ],
        compiler_params=pltpu.CompilerParams(
            collective_id=1, has_side_effects=True, vmem_limit_bytes=LIMIT
        ),
    )(samples, labels)
    return pl.pallas_call(
        functools.partial(finish, blk * slots, perms),
        out_shape=(
            jax.ShapeDtypeStruct((qr, 128), F32),
            jax.ShapeDtypeStruct((1, blk), F32),
            jax.ShapeDtypeStruct((1, 1), F32),
        ),
        in_specs=[vm],
        out_specs=(vm, vm, vm),
    )(res)


def solution(mesh):
    n_row, n_col = mesh.shape["row"], mesh.shape["col"]

    def shards(samples, labels):
        blk, width = samples.shape
        perms = labels.shape[1]
        pn = Plan(n_row, n_col, blk, width, perms)
        n_send = send_count(pn)
        n_lev, nz = pn.n_lev, pn.nz
        if (pn.nx, pn.ny, pn.nk, nz, blk) == (2, 2, 2, 4, 128):
            stat, proof, p = line_call(samples, labels)
            return stat.reshape(perms), proof.reshape(blk), p.reshape(())
        msg = perms // 128 + 2
        slots = n_row * n_col if pn.direct else n_lev
        vm = pl.BlockSpec(memory_space=pltpu.VMEM)
        hbm = pl.BlockSpec(memory_space=pl.ANY)
        dma = pltpu.SemaphoreType.DMA
        stat, proof, p = pl.pallas_call(
            functools.partial(kernel, pn, n_send),
            out_shape=(
                jax.ShapeDtypeStruct((perms // 128, 128), F32),
                jax.ShapeDtypeStruct((1, blk), F32),
                jax.ShapeDtypeStruct((1, 1), F32),
            ),
            in_specs=[hbm, hbm],
            out_specs=(vm, vm, vm),
            scratch_shapes=[
                pltpu.VMEM((blk, width), F32),
                pltpu.VMEM((blk, perms), jnp.int32),
                pltpu.VMEM((n_lev, blk, width), F32),
                pltpu.VMEM((n_lev, blk, perms), jnp.int32),
                pltpu.VMEM((nz, blk, width), F32),
                pltpu.VMEM((nz, blk, perms), jnp.int32),
                pltpu.VMEM((n_lev * blk, width), BF16),
                pltpu.VMEM((n_lev * blk, width), BF16),
                pltpu.VMEM((n_lev * blk, perms), BF16),
                pltpu.VMEM((1, n_lev * blk), F32),
                pltpu.VMEM((1, n_lev * blk), F32),
                pltpu.VMEM((nz + 1, blk, perms), F32),
                pltpu.VMEM((nz + 1, perms), F32),
                pltpu.VMEM((nz + 1, blk), F32),
                pltpu.VMEM((nz + 1, blk), F32),
                pltpu.VMEM((n_lev, msg, 128), F32),
                pltpu.VMEM((slots, msg, 128), F32),
                pltpu.VMEM((nz + 1, msg, 128), F32),
                pltpu.VMEM((nz, msg, 128), F32),
                dma((2,)),
                dma((n_send,)),
                dma((n_lev, 2 * PARTS)),
                dma((nz, 2 * CHUNKS)),
                dma((slots,)),
                dma((slots,)),
                dma((nz,)),
                dma((nz,)),
                pltpu.SemaphoreType.REGULAR,
            ],
            compiler_params=pltpu.CompilerParams(
                collective_id=0, has_side_effects=True, vmem_limit_bytes=60 * 1024 * 1024
            ),
        )(samples, labels)
        return stat.reshape(perms), proof.reshape(blk), p.reshape(())

    placed = (P(("row", "col"), None), P(("row", "col"), None))
    return jax.shard_map(
        shards, mesh=mesh, in_specs=placed, out_specs=(P(), P(("row", "col")), P()), check_vma=False
    )
```

```python
import functools
import math

import jax
import jax.numpy as jnp
from jax import lax
from jax.experimental import pallas as pl
from jax.experimental.pallas import tpu as pltpu
from jax.sharding import PartitionSpec as P

MESH = pl.DeviceIdType.MESH
F32 = jnp.float32
BF16 = jnp.bfloat16
CHUNKS = 4
PARTS = 2
LIMIT = 60 * 1024 * 1024

ROUTES = {1: {}, 2: {0: (1, 1)}, 4: {0: (1, 3), 2: (-1, 1), 3: (-1, 2)}}


def nt(a, b):
    return lax.dot_general(a, b, (((1,), (1,)), ((), ())), preferred_element_type=F32)


def nn(a, b):
    return lax.dot_general(a, b, (((1,), (0,)), ((), ())), preferred_element_type=F32)


def split(v):
    hi = v.astype(BF16)
    return hi, (v - hi.astype(F32)).astype(BF16)


def to_row(column):
    n = column.shape[0]
    return jnp.transpose(jnp.broadcast_to(column, (n, n)))[0:1, :]


class Plan:
    def __init__(self, n_row, n_col, blk, width, perms):
        self.nz = math.gcd(n_row, 4)
        self.nx = n_row // self.nz
        self.nk = math.gcd(n_col, 2)
        self.ny = n_col // self.nk
        self.n_col = n_col
        self.n_lev = self.nx * n_col
        self.blk, self.width, self.perms = blk, width, perms
        self.direct = n_row * n_col <= 32
        self.group = math.gcd(n_col, 4)
        self.rows = blk * n_row * n_col


def kernel(pn, n_send, x_hbm, l_hbm, stat_ref, proof_ref, p_ref, x_ref, l_ref, RX, RL, CX, CL, RHI, RLO, RLB, NR,
           ROWP, PROJ, QUAD, TOT, COLP, S1, R1, S2, R2, in_sem, send, lev_sem, z_sem, s1_send, s1_recv, s2_send, s2_recv, here):
    nx, ny, nz, nk, n_col, n_lev, blk = pn.nx, pn.ny, pn.nz, pn.nk, pn.n_col, pn.n_lev, pn.blk
    row, col = lax.axis_index("row"), lax.axis_index("col")
    z, x = row // nx, row % nx
    y, core = col // nk, col % nk
    me = x * n_col + col
    routes = ROUTES[nz]
    pending = []

    def lev_of(xx, yy, kk):
        return xx * n_col + yy * nk + kk

    def dev(zz, xx, yy, kk):
        return (zz * nx + xx, yy * nk + kk)

    def lev_dev(k):
        return (z * nx + k // n_col, k % n_col)

    loads = [pltpu.make_async_copy(x_hbm, x_ref, in_sem.at[0]), pltpu.make_async_copy(l_hbm, l_ref, in_sem.at[1])]
    for c in loads:
        c.start()
    barrier = pltpu.get_barrier_semaphore()
    for d in range(1, n_lev):
        pl.semaphore_signal(barrier, inc=1, device_id=lev_dev((me + d) % n_lev), device_id_type=MESH)
    for d in range(1, nz):
        pl.semaphore_signal(barrier, inc=1, device_id=dev((z + d) % nz, x, y, core), device_id_type=MESH)
    pl.semaphore_wait(barrier, n_lev - 1 + nz - 1)
    for c in loads:
        c.wait()

    n_dev = nz * n_lev
    direct = pn.direct
    if direct:
        for d in range(1, nz):
            pl.semaphore_signal(here, inc=1, device_id=dev((z + d) % nz, x, y, core), device_id_type=MESH)

    counter = [0]

    def new_sem():
        counter[0] += 1
        return send.at[counter[0] - 1]

    half = blk // PARTS
    piece = blk // CHUNKS

    def lev_copy(k, part, target, own, sem):
        r = pl.ds(part * half, half)
        out = []
        for i, (src, dst) in enumerate(((x_ref, RX), (l_ref, RL))):
            s = src.at[r] if own else dst.at[k, r]
            out.append(pltpu.make_async_remote_copy(
                src_ref=s, dst_ref=dst.at[k, r], send_sem=new_sem() if sem else send.at[0],
                recv_sem=lev_sem.at[k, part * 2 + i], device_id=target, device_id_type=MESH))
        return out

    def lev_send(k, part, target, own=False):
        for c in lev_copy(k, part, target, own, True):
            c.start()
            pending.append(c)

    def lev_wait(k, part):
        for c in lev_copy(k, part, (row, col), False, False):
            c.wait_recv()

    def z_copy(b, ch, target, own, sems):
        r = pl.ds(ch * piece, piece)
        out = []
        for i, (src, dst) in enumerate(((x_ref, CX), (l_ref, CL))):
            s = src.at[r] if own else dst.at[b, r]
            out.append(pltpu.make_async_remote_copy(
                src_ref=s, dst_ref=dst.at[b, r], send_sem=sems[i],
                recv_sem=z_sem.at[b, ch * 2 + i], device_id=target, device_id_type=MESH))
        return out

    z_pending = []

    def z_send(b, ch, at, own):
        sems = [new_sem(), new_sem()]
        to = at + routes[b][0]

        @pl.when(z == at)
        def _():
            for c in z_copy(b, ch, dev(to, x, y, core), own, sems):
                c.start()
        z_pending.append((b, ch, at, own, sems))

    def z_arrive(b, ch, at):
        for c in z_copy(b, ch, (row, col), False, [send.at[0]] * 2):
            c.wait_recv()

    def z_round(hop, ch):
        for b in routes:
            if hop < routes[b][1]:
                at = b + routes[b][0] * hop

                @pl.when(z == at)
                def _():
                    z_arrive(b, ch, at)
                z_send(b, ch, at, False)

    def xm(d):
        return (x + d) % nx

    def ym(d):
        return (y + d) % ny

    other = (core + 1) % nk
    A, B = 0, 1
    for ch in range(CHUNKS):
        for b in routes:
            z_send(b, ch, b, True)
    for d in range(1, nx):
        lev_send(me, A, dev(z, xm(d), y, core), True)
    for d in range(1, ny):
        lev_send(me, B, dev(z, x, ym(d), core), True)
    for d in range(1, nx):
        lev_send(me, B, dev(z, xm(d), y, core), True)
    for d in range(1, ny):
        lev_send(me, A, dev(z, x, ym(d), core), True)
    if nk > 1:
        for part in (A, B):
            lev_send(me, part, dev(z, x, y, other), True)

    def prep(k, xv, lv):
        rows = pl.ds(pl.multiple_of(k * blk, blk), blk)
        hi, lo = split(xv)
        RHI[rows, :] = hi
        RLO[rows, :] = lo
        RLB[rows, :] = lv.astype(F32).astype(BF16)
        NR[:, rows] = to_row(jnp.sum(xv * xv, axis=1, keepdims=True))

    def prep_chunk(xx, skip):
        def step(i, _):
            k = xx * n_col + (col + i) % n_col
            prep(k, RX[k], RL[k])
            return 0

        lax.fori_loop(skip, n_col, step, 0)

    span = pn.group * blk
    scale = -1.0 / (2.0 * pn.width)

    def tile(slot, xx, xv, lv, own):
        chi, clo = split(xv)
        nc = jnp.sum(xv * xv, axis=1, keepdims=True)
        l0 = lv[:, 0:1].astype(F32)
        proj = PROJ[slot]
        tot = TOT[slot:slot + 1, :]
        for j in range(n_col // pn.group):
            base = pl.multiple_of(xx * n_col * blk + j * span, span)
            rows = pl.ds(base, span)
            hi, lo, lb = RHI[rows, :], RLO[rows, :], RLB[rows, :]
            dots = nt(chi, hi) + nt(chi, lo) + nt(clo, hi)
            dist = jnp.maximum(nc + NR[:, rows] - 2.0 * dots, 0.0)
            kern = jnp.exp(dist * scale)
            if own:
                ids = lax.broadcasted_iota(jnp.int32, (blk, span), 1) + base
                mine = lax.broadcasted_iota(jnp.int32, (blk, span), 0) + me * blk
                kern = jnp.where(ids == mine, 0.0, kern)
            kh, kl = split(kern)
            proj = proj + nn(kh, lb) + nn(kl, lb)
            t = jnp.sum(kern, axis=0, keepdims=True)
            for g in range(pn.group):
                tot = tot + t[:, g * blk:(g + 1) * blk]
            if not own:
                ROWP[:, rows] += jnp.sum(kern * l0, axis=0, keepdims=True)
        PROJ[slot] = proj
        TOT[slot:slot + 1, :] = tot

    def line_tiles(hop, chunks, arrive):
        for b in routes:
            if hop <= routes[b][1]:
                at = b + routes[b][0] * hop

                @pl.when(z == at)
                def _():
                    if arrive and hop == routes[b][1]:
                        for ch in range(CHUNKS):
                            z_arrive(b, ch, at)
                    for xx in chunks:
                        tile(b, xx, CX[b], CL[b], False)

    def own_tile(xx):
        tile(nz, xx, x_ref[...], l_ref[...], True)

    prep(me, x_ref[...], l_ref[...])
    ROWP[...] = jnp.zeros_like(ROWP)
    PROJ[...] = jnp.zeros_like(PROJ)
    TOT[...] = jnp.zeros_like(TOT)

    def partner(k, part):
        if nk > 1:
            lev_send(k, part, dev(z, x, y, other))

    z_round(1, 0)
    for d in range(1, nx):
        k = lev_of(xm(d), y, core)
        lev_wait(k, A)
        for e in range(1, ny):
            lev_send(k, A, dev(z, x, ym(e), core))
        partner(k, A)
    for d in range(1, ny):
        k = lev_of(x, ym(d), core)
        lev_wait(k, B)
        for e in range(1, nx):
            lev_send(k, B, dev(z, xm(e), y, core))
        partner(k, B)
    z_round(1, 1)
    z_round(2, 0)
    z_round(1, 2)
    z_round(2, 1)
    z_round(1, 3)
    for d in range(1, ny):
        k = lev_of(x, ym(d), core)
        lev_wait(k, A)
        partner(k, A)
    for d in range(1, nx):
        k = lev_of(xm(d), y, core)
        lev_wait(k, B)
        partner(k, B)
    z_round(2, 2)

    def other_core(xx, ys):
        if nk > 1:
            for e in ys:
                for part in (A, B):
                    lev_wait(lev_of(xx, ym(e), other), part)

    other_core(x, range(ny))
    prep_chunk(x, 1)
    own_tile(x)
    z_round(2, 3)
    line_tiles(1, [x], True)
    for d in range(1, nx):
        for e in range(1, ny):
            k = lev_of(xm(d), ym(e), core)
            for part in (A, B):
                lev_wait(k, part)
                partner(k, part)
    far = [xm(d) for d in range(1, nx)]
    for xx in far:
        other_core(xx, range(ny))
        prep_chunk(xx, 0)
        own_tile(xx)
    line_tiles(1, far, False)
    for hop in range(2, nz):
        line_tiles(hop, [x] + far, True)

    quad = jnp.zeros((1, pn.perms), F32)
    tot = jnp.zeros((1, blk), F32)
    for b in list(routes) + [nz]:
        w = 1.0 if b == nz else 2.0
        lv = l_ref[...] if b == nz else CL[b]
        QUAD[b:b + 1, :] = jnp.zeros((1, pn.perms), F32)
        COLP[b:b + 1, :] = jnp.zeros((1, blk), F32)
        reach = [nz - 1] if b == nz else [b + routes[b][0] * h for h in range(1, routes[b][1] + 1)]

        @pl.when((z >= (0 if b == nz else min(reach))) & (z <= max(reach)))
        def _():
            QUAD[b:b + 1, :] = w * jnp.sum(lv.astype(F32) * PROJ[b], axis=0, keepdims=True)
            COLP[b:b + 1, :] = to_row(PROJ[b][:, 0:1])
        quad = quad + QUAD[b:b + 1, :]
        tot = tot + w * TOT[b:b + 1, :]
    own_proof = COLP[nz:nz + 1, :]

    qr = pn.perms // 128
    if direct:
        def head(ref, i):
            for j in range(qr):
                ref[i, j:j + 1, :] = quad[:, j * 128:(j + 1) * 128]
            ref[i, qr:qr + 1, :] = tot

        index = z * n_lev + me
        none = jnp.zeros((1, 128), F32)
        for k in range(n_lev):
            head(S1, k)
            S1[k, qr + 1:qr + 2, :] = ROWP[:, k * blk:(k + 1) * blk]
        for b in range(nz):
            head(S2, b)
            S2[b, qr + 1:qr + 2, :] = COLP[b:b + 1, :] if b in routes else none
        head(S2, nz)
        S2[nz, qr + 1:qr + 2, :] = none
        if nz > 1:
            pl.semaphore_wait(here, nz - 1)

        def x_copy(dz, d, slot):
            b, k = (z + dz) % nz, (me + d) % n_lev
            src = S1.at[k] if dz == 0 else (S2.at[b] if d == 0 else S2.at[nz])
            return pltpu.make_async_remote_copy(
                src_ref=src, dst_ref=R1.at[slot], send_sem=s1_send.at[dz * n_lev + d], recv_sem=s1_recv.at[slot],
                device_id=(b * nx + k // n_col, k % n_col), device_id_type=MESH)

        pairs = [(dz, d) for dz in reversed(range(nz)) for d in range(n_lev) if dz + d > 0]
        for dz, d in pairs:
            x_copy(dz, d, index).start()
        R1[index] = S1[me]
        for dz, d in pairs:
            x_copy(dz, d, ((z + dz) % nz) * n_lev + (me + d) % n_lev).wait_recv()
        done = R1[0]
        for i in range(1, n_dev):
            done = done + R1[i]
        proof = done[qr + 1:qr + 2, :] + own_proof
    else:
        for k in range(n_lev):
            for i in range(qr):
                S1[k, i:i + 1, :] = quad[:, i * 128:(i + 1) * 128]
            S1[k, qr:qr + 1, :] = tot
            S1[k, qr + 1:qr + 2, :] = ROWP[:, k * blk:(k + 1) * blk]

        def s1_copy(d):
            k = (me + d) % n_lev
            return pltpu.make_async_remote_copy(
                src_ref=S1.at[k], dst_ref=R1.at[me], send_sem=s1_send.at[k], recv_sem=s1_recv.at[me],
                device_id=lev_dev(k), device_id_type=MESH)

        def s1_in(d):
            k = (me + d) % n_lev
            return pltpu.make_async_remote_copy(
                src_ref=S1.at[k], dst_ref=R1.at[k], send_sem=s1_send.at[k], recv_sem=s1_recv.at[k],
                device_id=lev_dev(k), device_id_type=MESH)

        for d in range(1, n_lev):
            s1_copy(d).start()
        acc = S1[me]
        for d in range(1, n_lev):
            s1_in(d).wait_recv()
            acc = acc + R1[(me + d) % n_lev]
        for b in range(nz):
            S2[b, :, :] = acc
            S2[b, qr + 1:qr + 2, :] = COLP[b:b + 1, :] if b in routes else jnp.zeros((1, 128), F32)

        def s2_copy(d):
            b = (z + d) % nz
            return pltpu.make_async_remote_copy(
                src_ref=S2.at[b], dst_ref=R2.at[z], send_sem=s2_send.at[b], recv_sem=s2_recv.at[z],
                device_id=dev(b, x, y, core), device_id_type=MESH)

        def s2_in(d):
            b = (z + d) % nz
            return pltpu.make_async_remote_copy(
                src_ref=S2.at[b], dst_ref=R2.at[b], send_sem=s2_send.at[b], recv_sem=s2_recv.at[b],
                device_id=dev(b, x, y, core), device_id_type=MESH)

        for d in range(1, nz):
            s2_copy(d).start()
        for d in range(1, nz):
            s2_in(d).wait_recv()
        tops = []
        extra = jnp.zeros((1, 128), F32)
        for b in range(nz):
            mine = z == b
            tops.append(jnp.where(mine, acc, R2[b]))
            extra = extra + jnp.where(mine, 0.0, R2[b, qr + 1:qr + 2, :])
        done = functools.reduce(lambda u, v: u + v, tops)
        proof = acc[qr + 1:qr + 2, :] + own_proof + extra
    total = jnp.sum(done[qr:qr + 1, :], axis=1, keepdims=True)
    hf = pn.rows / 2.0
    den = 2.0 * hf * (hf - 1.0)
    stat = total / den + ((2.0 * hf - 1.0) / den) * done[0:qr, :]
    stat_ref[...] = stat
    proof_ref[...] = proof / math.sqrt(pn.rows)
    sg = 1.0 / (1.0 + jnp.exp(-4.0 * (stat - stat[0:1, 0:1])))
    first = (lax.broadcasted_iota(jnp.int32, stat.shape, 0) + lax.broadcasted_iota(jnp.int32, stat.shape, 1)) == 0
    sg = jnp.where(first, 0.0, sg)
    p = jnp.sum(jnp.sum(sg, axis=0, keepdims=True), axis=1, keepdims=True) / (pn.perms - 1)
    p_ref[...] = p

    for c in pending:
        c.wait_send()
    for b, ch, at, own, sems in z_pending:
        @pl.when(z == at)
        def _():
            for c in z_copy(b, ch, dev(at + routes[b][0], x, y, core), own, sems):
                c.wait_send()
    if direct:
        for dz, d in pairs:
            x_copy(dz, d, index).wait_send()
    else:
        for d in range(1, n_lev):
            s1_copy(d).wait_send()
        for d in range(1, nz):
            s2_copy(d).wait_send()
    assert counter[0] == n_send


def send_count(pn):
    nx, ny, nk, nz = pn.nx, pn.ny, pn.nk, pn.nz
    own = 2 * (nx - 1) + 2 * (ny - 1) + (2 if nk > 1 else 0)
    fwd = 2 * (nx - 1) * (ny - 1)
    core = 2 * (nx * ny - 1) if nk > 1 else 0
    line = sum(h for _, h in ROUTES[nz].values()) * CHUNKS
    return 2 * (own + fwd + core + line)


def line_kernel(x_hbm, l_hbm, out_ref, x_ref, l_ref, GX, GL, CX, CL, CC, HI, LO, LB, SH, SL, NR, NC, L0, OWN0,
                ROWP, PROJ, TOT, S1, R1, in_sem, xy_send, xy_recv, z_send, z_recv, m_send, m_recv, line, here):
    blk, width = x_ref.shape
    perms = l_ref.shape[1]
    nx, ny, nk, nz, n_lev = 2, 2, 2, 4, 8
    row, col = lax.axis_index("row"), lax.axis_index("col")
    z, x = row // nx, row % nx
    y, core = col // nk, col % nk
    qr = perms // 128
    A, B, ALL = 0, 1, 2

    def dev(zz, xx, yy, kk):
        return (zz * nx + xx, yy * nk + kk)

    def signal(sem, to):
        pl.semaphore_signal(sem, inc=1, device_id=to, device_id_type=MESH)

    def remote(src, dst, ss, rs, to):
        return pltpu.make_async_remote_copy(src_ref=src, dst_ref=dst, send_sem=ss, recv_sem=rs, device_id=to,
                                            device_id_type=MESH)

    here_dev = (row, col)
    x_dev, y_dev, k_dev = dev(z, 1 - x, y, core), dev(z, x, 1 - y, core), dev(z, x, y, 1 - core)
    place = [(xx, yy, kk) for xx, yy, kk in ((x, y, core), (x, y, 1 - core), (1 - x, y, core), (x, 1 - y, core),
             (1 - x, y, 1 - core), (x, 1 - y, 1 - core), (1 - x, 1 - y, core), (1 - x, 1 - y, 1 - core))]

    loads = [pltpu.make_async_copy(x_hbm, x_ref, in_sem.at[0]), pltpu.make_async_copy(l_hbm, l_ref, in_sem.at[1])]
    for c in loads:
        c.start()
    barrier = pltpu.get_barrier_semaphore()
    for to in (x_dev, y_dev, k_dev):
        signal(barrier, to)

    @pl.when(z == 1)
    def _():
        signal(barrier, dev(0, x, y, core))

    @pl.when((z == 1) | (z == 2))
    def _():
        signal(barrier, dev(z + 1, x, y, core))

    ROWP[...] = jnp.zeros_like(ROWP)
    PROJ[...] = jnp.zeros_like(PROJ)
    TOT[...] = jnp.zeros_like(TOT)
    for c in reversed(loads):
        c.wait()
    OWN0[...] = to_row(l_ref[:, 0:1].astype(F32)).astype(jnp.int32)
    pl.semaphore_wait(barrier, jnp.where(z == 1, 3, 4))

    half = blk // 2

    def xy_copy(src, dst, part, i, to):
        r = pl.ds(part * half, half) if part < 2 else pl.ds(0, blk)
        mine, buf = ((x_ref, GX), (l_ref, GL))[i]
        s = mine.at[r] if src == 0 else buf.at[src, r]
        n = part % 2 * 2 + i
        return remote(s, buf.at[dst, r], xy_send.at[dst, n], xy_recv.at[dst, n], to)

    sent = []
    X, L = 0, 1

    def xy_start(src, dst, part, to, kinds=(X, L)):
        for i in kinds:
            c = xy_copy(src, dst, part, i, to)
            c.start()
            sent.append(c)

    def xy_wait(at, parts=(A, B), kinds=(X, L)):
        for part in parts:
            for i in kinds:
                xy_copy(at, at, part, i, here_dev).wait_recv()

    piece = blk // 4
    SAM, LAB = [0, 1, 2, 3], [5, 6, 7, 8]

    EACH = {p: (p % 5, p % 5 + 1) for p in SAM + LAB}
    WHOLE = {3: (0, 4), 8: (0, 4)}
    CUTS = {0: EACH, 2: WHOLE, 3: {1: (0, 2), 3: (2, 4), 8: (0, 4)}}

    def held(b, ps):
        return [p for p in ps if p == 4 or p in CUTS[b]]

    def z_copy(b, p, own, to):
        if p == 4:
            src, dst = (OWN0 if own else CC.at[b]), CC.at[b]
        else:
            first, end = CUTS[b][p]
            r = pl.ds(first * piece, (end - first) * piece)
            mine, buf = (x_ref, CX) if p < 4 else (l_ref, CL)
            src, dst = (mine.at[r] if own else buf.at[b, r]), buf.at[b, r]
        return remote(src, dst, z_send.at[b, p], z_recv.at[b, p], to)

    def z_start(b, ps, own, step):
        for p in held(b, ps):
            z_copy(b, p, own, dev(z + step, x, y, core)).start()

    def z_wait(b, ps):
        for p in held(b, ps):
            z_copy(b, p, False, here_dev).wait_recv()

    def z_pass(b, ps, step):
        for p in held(b, ps):
            z_wait(b, [p])
            z_start(b, [p], False, step)

    def at_z(*levels):
        cond = z == levels[0]
        for v in levels[1:]:
            cond = cond | (z == v)
        return pl.when(cond)

    @at_z(0)
    def _():
        z_start(0, SAM + [4] + LAB, True, 1)
        signal(line, dev(1, x, y, core))

    @at_z(2)
    def _():
        z_start(2, SAM + [4], True, -1)

    @at_z(3)
    def _():
        z_start(3, SAM + [4] + LAB, True, -1)
        signal(line, dev(2, x, y, core))

    xy_start(0, 2, A, x_dev)
    xy_start(0, 3, B, y_dev)
    xy_start(0, 2, B, x_dev)
    xy_start(0, 3, A, y_dev)
    xy_start(0, 1, ALL, k_dev)

    scale = -1.0 / (2.0 * width)
    span = nk * blk

    order = {0: [], 1: [0, 2, 3], 2: [3, 0], 3: [0]}

    def norms(v):
        return jnp.sum(v * v, axis=1, keepdims=True)

    def prep(at, v, lv):
        hi, lo = split(v)
        n = norms(v)
        rows = slice(at * blk, (at + 1) * blk)
        HI[rows, :] = hi
        LO[rows, :] = lo
        LB[rows, :] = lv.astype(F32).astype(BF16)
        NR[:, rows] = to_row(n)
        if at == 0:
            SH[rows, :] = hi
            SL[rows, :] = lo
            NC[rows, :] = n

    def prep_at(at):
        prep(at, GX[at], GL[at])

    def prep_line(b, j):
        hi, lo = split(CX[b])
        rows = slice(j * blk, (j + 1) * blk)
        SH[rows, :] = hi
        SL[rows, :] = lo
        NC[rows, :] = norms(CX[b])
        L0[rows, :] = jnp.transpose(jnp.broadcast_to(CC[b], (blk, blk)))[:, 0:1].astype(F32)

    def work(j0, j1, *groups):
        mine = slice(j0 * blk, j1 * blk)
        n = (j1 - j0) * blk
        tiles = []
        for g in groups:
            rows = slice(g * span, (g + 1) * span)
            hi = SH[mine, :]
            d = nt(jnp.concatenate([hi, SL[mine, :]], axis=0), HI[rows, :])
            tiles.append((g, rows, d[:n] + d[n:] + nt(hi, LO[rows, :])))
        for g, rows, dots in tiles:
            dist = jnp.maximum(NC[mine, :] + NR[:, rows] - 2.0 * dots, 0.0)
            kern = jnp.exp(dist * scale)
            if j0 == 0:
                top = kern[:blk]
                if g == 0:
                    gap = lax.broadcasted_iota(jnp.int32, top.shape, 1) - lax.broadcasted_iota(jnp.int32, top.shape, 0)
                    top = jnp.where(gap == 0, 0.0, top)
                    kern = top if n == blk else jnp.concatenate([top, kern[blk:]], axis=0)
                t = jnp.sum(top, axis=0, keepdims=True)
            else:
                t = jnp.zeros((1, span), F32)
            kh, kl = split(kern)
            p = nn(jnp.concatenate([kh, kl], axis=0), LB[rows, :])
            PROJ[mine, :] += p[:n] + p[n:]
            rest = kern[blk:] if j0 == 0 else kern
            if rest.shape[0]:
                t = t + 2.0 * jnp.sum(rest, axis=0, keepdims=True)
                line_rows = slice(max(j0, 1) * blk, j1 * blk)
                ROWP[:, rows] += jnp.sum(rest * L0[line_rows, :], axis=0, keepdims=True)
            TOT[...] += t[:, :blk] + t[:, blk:]

    prep(0, x_ref[...], l_ref[...])

    @at_z(2)
    def _():
        pl.semaphore_wait(line, 1)
        signal(line, dev(1, x, y, core))

    xy_wait(1, (ALL,))
    prep_at(1)

    @at_z(0, 3)
    def _():
        work(0, 1, 0)

    @at_z(1)
    def _():
        pl.semaphore_wait(line, 2)
        signal(line, dev(0, x, y, core))
        signal(line, dev(2, x, y, core))
        z_pass(0, [0, 1, 2], 1)

    @at_z(2)
    def _():
        z_pass(3, [0, 1], -1)
        pl.semaphore_wait(line, 1)
        signal(line, dev(3, x, y, core))
        z_pass(3, [2], -1)

    xy_wait(2, (A,))
    xy_start(2, 6, A, y_dev)
    xy_start(2, 4, A, k_dev)
    xy_wait(3, (B,))
    xy_start(3, 6, B, x_dev)
    xy_start(3, 5, B, k_dev)

    @at_z(1)
    def _():
        z_pass(0, [3, 4], 1)
        prep_line(0, 1)
        z_wait(2, SAM + [4])
        prep_line(2, 2)
        work(0, 3, 0)
        z_pass(0, LAB, 1)

    @at_z(2)
    def _():
        z_pass(3, [3, 4], -1)
        z_start(2, LAB, True, -1)
        prep_line(3, 1)
        z_pass(0, [0], 1)
        work(0, 2, 0)
        z_pass(0, [1], 1)
        z_pass(3, LAB[:3], -1)
        z_pass(0, [2], 1)
        z_pass(3, LAB[3:], -1)

    xy_wait(2, (B,))
    xy_start(2, 4, B, k_dev)
    xy_wait(3, (A,))
    xy_start(3, 5, A, k_dev)

    @at_z(0, 3)
    def _():
        pl.semaphore_wait(line, 1)

    signal(here.at[0], k_dev)
    prep_at(2)
    prep_at(3)

    @at_z(0, 3)
    def _():
        work(0, 1, 1)

    @at_z(1)
    def _():
        work(0, 3, 1)

    @at_z(2)
    def _():
        work(0, 2, 1)
        z_pass(0, [3, 4], 1)
        prep_line(0, 2)

    xy_wait(4)
    xy_wait(5)
    pl.semaphore_wait(here.at[0], 1)
    signal(here.at[1], x_dev)
    prep_at(4)
    prep_at(5)

    @at_z(0, 3)
    def _():
        work(0, 1, 2)

    @at_z(1)
    def _():
        work(0, 3, 2)

    @at_z(2)
    def _():
        work(0, 2, 2)
        z_pass(0, LAB[:2], 1)

    xy_wait(6, (A, B), (X,))
    xy_start(6, 7, ALL, k_dev, (X,))
    pl.semaphore_wait(here.at[1], 1)
    signal(here.at[2], y_dev)

    @at_z(1)
    def _():
        z_wait(3, SAM + [4])
        prep_line(3, 3)
        work(3, 4, 0, 1, 2)

    xy_wait(6, (A, B), (L,))
    xy_start(6, 7, ALL, k_dev, (L,))

    @at_z(2)
    def _():
        z_pass(0, LAB[2:], 1)
        work(2, 3, 0, 1, 2)

    prep_at(6)

    @at_z(3)
    def _():
        z_wait(0, SAM + [4])
        prep_line(0, 1)
        work(1, 2, 0, 1, 2)

    xy_wait(7, (ALL,))
    prep_at(7)
    for level in range(nz):
        @at_z(level)
        def _():
            work(0, 1 + len(order[level]), 3)

    def proj(j):
        return PROJ[j * blk:(j + 1) * blk, :]

    none = jnp.zeros((1, 128), F32)
    own_proof = to_row(proj(0)[:, 0:1])
    tot = TOT[...]
    for i in range(n_lev):
        S1[i, qr:qr + 1, :] = tot
        S1[i, qr + 1:qr + 2, :] = ROWP[:, i * blk:(i + 1) * blk]
    for b in range(nz + 1):
        S1[n_lev + b, qr:qr + 1, :] = tot
        S1[n_lev + b, qr + 1:qr + 2, :] = none
    for level in range(1, nz):
        @at_z(level)
        def _():
            for j, b in enumerate(order[level]):
                S1[n_lev + b, qr + 1:qr + 2, :] = to_row(proj(j + 1)[:, 0:1])

    def add(w, j, lv):
        q = w * jnp.sum(lv.astype(F32) * proj(j), axis=0, keepdims=True)
        for i in range(qr):
            S1[n_lev + nz, i:i + 1, :] += q[:, i * 128:(i + 1) * 128]

    S1[n_lev + nz, 0:qr, :] = jnp.zeros((qr, 128), F32)
    add(1.0, 0, l_ref[...])

    @at_z(3)
    def _():
        z_wait(0, LAB)

    @at_z(1, 3)
    def _():
        add(2.0, 1, CL[0])

    @at_z(2)
    def _():
        add(2.0, 1, CL[3])
        add(2.0, 2, CL[0])

    @at_z(1)
    def _():
        z_wait(2, LAB)
        add(2.0, 2, CL[2])
        z_wait(3, LAB)
        add(2.0, 3, CL[3])

    q = S1[n_lev + nz, 0:qr, :]
    for i in range(n_lev):
        S1[i, 0:qr, :] = q
    for b in range(nz):
        S1[n_lev + b, 0:qr, :] = q
    index = z * n_lev + x * 4 + col
    pl.semaphore_wait(here.at[2], 1)

    def m_copy(t, incoming):
        tz, tx, ty, tk = t // n_lev, t // 4 % nx, t // nk % ny, t % nk
        dx, dy, dk = jnp.where(tx == x, 0, 1), jnp.where(ty == y, 0, 1), jnp.where(tk == core, 0, 1)
        i = jnp.where(dk == 0, 2 * dx + 3 * dy + dx * dy, jnp.where(dx + dy == 0, 1, 3 + dx + 2 * dy + dx * dy))
        n = jnp.where(tz == z, i, n_lev + jnp.where(i == 0, tz, nz))
        return remote(S1.at[n], R1.at[t if incoming else index], m_send.at[t], m_recv.at[t if incoming else index],
                      dev(tz, tx, ty, tk))

    def others(act):
        for t in range(nz * n_lev):
            @pl.when(t != index)
            def _():
                act(t)

    others(lambda t: m_copy(t, False).start())
    R1[index] = S1[0]

    for c in sent:
        c.wait_send()
    for at, b in ((0, 0), (1, 0), (2, 0), (2, 2), (2, 3), (3, 3)):
        @at_z(at)
        def _():
            for p in held(b, SAM + [4] + LAB):
                z_copy(b, p, False, here_dev).wait_send()

    others(lambda t: m_copy(t, False).wait_send())
    done = jnp.zeros((qr + 2, 128), F32)
    for t in range(nz * n_lev):
        @pl.when(t != index)
        def _():
            m_copy(t, True).wait_recv()
        done = done + R1[t]
    out_ref[0:qr + 1, :] = done[0:qr + 1, :]
    out_ref[qr + 1:qr + 2, :] = done[qr + 1:qr + 2, :] + own_proof


def finish(rows, perms, r_ref, stat_ref, proof_ref, p_ref):
    qr = perms // 128
    total = jnp.sum(r_ref[qr:qr + 1, :], axis=1, keepdims=True)
    hf = rows / 2.0
    den = 2.0 * hf * (hf - 1.0)
    stat = total / den + ((2.0 * hf - 1.0) / den) * r_ref[0:qr, :]
    stat_ref[...] = stat
    proof_ref[...] = r_ref[qr + 1:qr + 2, :] / math.sqrt(rows)
    sg = 1.0 / (1.0 + jnp.exp(-4.0 * (stat - stat[0:1, 0:1])))
    first = (lax.broadcasted_iota(jnp.int32, stat.shape, 0) + lax.broadcasted_iota(jnp.int32, stat.shape, 1)) == 0
    sg = jnp.where(first, 0.0, sg)
    p_ref[...] = jnp.sum(jnp.sum(sg, axis=0, keepdims=True), axis=1, keepdims=True) / (perms - 1)


def line_call(samples, labels):
    blk, width = samples.shape
    perms = labels.shape[1]
    qr = perms // 128
    nz, n_lev = 4, 8
    slots = nz * n_lev
    i32 = jnp.int32
    dma = pltpu.SemaphoreType.DMA
    vm = pl.BlockSpec(memory_space=pltpu.VMEM)
    hbm = pl.BlockSpec(memory_space=pl.ANY)
    res = pl.pallas_call(
        line_kernel,
        out_shape=jax.ShapeDtypeStruct((qr + 2, 128), F32),
        in_specs=[hbm, hbm],
        out_specs=vm,
        scratch_shapes=[
            pltpu.VMEM((blk, width), F32),
            pltpu.VMEM((blk, perms), i32),
            pltpu.VMEM((n_lev, blk, width), F32),
            pltpu.VMEM((n_lev, blk, perms), i32),
            pltpu.VMEM((nz, blk, width), F32),
            pltpu.VMEM((nz, blk, perms), i32),
            pltpu.VMEM((nz, 1, blk), i32),
            pltpu.VMEM((n_lev * blk, width), BF16),
            pltpu.VMEM((n_lev * blk, width), BF16),
            pltpu.VMEM((n_lev * blk, perms), BF16),
            pltpu.VMEM((nz * blk, width), BF16),
            pltpu.VMEM((nz * blk, width), BF16),
            pltpu.VMEM((1, n_lev * blk), F32),
            pltpu.VMEM((nz * blk, 1), F32),
            pltpu.VMEM((nz * blk, 1), F32),
            pltpu.VMEM((1, blk), i32),
            pltpu.VMEM((1, n_lev * blk), F32),
            pltpu.VMEM((nz * blk, perms), F32),
            pltpu.VMEM((1, blk), F32),
            pltpu.VMEM((n_lev + nz + 1, qr + 2, 128), F32),
            pltpu.VMEM((slots, qr + 2, 128), F32),
            dma((2,)),
            dma((n_lev, 4)),
            dma((n_lev, 4)),
            dma((nz, 9)),
            dma((nz, 9)),
            dma((slots,)),
            dma((slots,)),
            pltpu.SemaphoreType.REGULAR,
            pltpu.SemaphoreType.REGULAR((3,)),
        ],
        compiler_params=pltpu.CompilerParams(
            collective_id=1, has_side_effects=True, vmem_limit_bytes=LIMIT
        ),
    )(samples, labels)
    return pl.pallas_call(
        functools.partial(finish, blk * slots, perms),
        out_shape=(
            jax.ShapeDtypeStruct((qr, 128), F32),
            jax.ShapeDtypeStruct((1, blk), F32),
            jax.ShapeDtypeStruct((1, 1), F32),
        ),
        in_specs=[vm],
        out_specs=(vm, vm, vm),
    )(res)


def solution(mesh):
    n_row, n_col = mesh.shape["row"], mesh.shape["col"]

    def shards(samples, labels):
        blk, width = samples.shape
        perms = labels.shape[1]
        pn = Plan(n_row, n_col, blk, width, perms)
        n_send = send_count(pn)
        n_lev, nz = pn.n_lev, pn.nz
        if (pn.nx, pn.ny, pn.nk, nz, blk) == (2, 2, 2, 4, 128):
            stat, proof, p = line_call(samples, labels)
            return stat.reshape(perms), proof.reshape(blk), p.reshape(())
        msg = perms // 128 + 2
        slots = n_row * n_col if pn.direct else n_lev
        vm = pl.BlockSpec(memory_space=pltpu.VMEM)
        hbm = pl.BlockSpec(memory_space=pl.ANY)
        dma = pltpu.SemaphoreType.DMA
        stat, proof, p = pl.pallas_call(
            functools.partial(kernel, pn, n_send),
            out_shape=(
                jax.ShapeDtypeStruct((perms // 128, 128), F32),
                jax.ShapeDtypeStruct((1, blk), F32),
                jax.ShapeDtypeStruct((1, 1), F32),
            ),
            in_specs=[hbm, hbm],
            out_specs=(vm, vm, vm),
            scratch_shapes=[
                pltpu.VMEM((blk, width), F32),
                pltpu.VMEM((blk, perms), jnp.int32),
                pltpu.VMEM((n_lev, blk, width), F32),
                pltpu.VMEM((n_lev, blk, perms), jnp.int32),
                pltpu.VMEM((nz, blk, width), F32),
                pltpu.VMEM((nz, blk, perms), jnp.int32),
                pltpu.VMEM((n_lev * blk, width), BF16),
                pltpu.VMEM((n_lev * blk, width), BF16),
                pltpu.VMEM((n_lev * blk, perms), BF16),
                pltpu.VMEM((1, n_lev * blk), F32),
                pltpu.VMEM((1, n_lev * blk), F32),
                pltpu.VMEM((nz + 1, blk, perms), F32),
                pltpu.VMEM((nz + 1, perms), F32),
                pltpu.VMEM((nz + 1, blk), F32),
                pltpu.VMEM((nz + 1, blk), F32),
                pltpu.VMEM((n_lev, msg, 128), F32),
                pltpu.VMEM((slots, msg, 128), F32),
                pltpu.VMEM((nz + 1, msg, 128), F32),
                pltpu.VMEM((nz, msg, 128), F32),
                dma((2,)),
                dma((n_send,)),
                dma((n_lev, 2 * PARTS)),
                dma((nz, 2 * CHUNKS)),
                dma((slots,)),
                dma((slots,)),
                dma((nz,)),
                dma((nz,)),
                pltpu.SemaphoreType.REGULAR,
            ],
            compiler_params=pltpu.CompilerParams(
                collective_id=0, has_side_effects=True, vmem_limit_bytes=60 * 1024 * 1024
            ),
        )(samples, labels)
        return stat.reshape(perms), proof.reshape(blk), p.reshape(())

    placed = (P(("row", "col"), None), P(("row", "col"), None))
    return jax.shard_map(
        shards, mesh=mesh, in_specs=placed, out_specs=(P(), P(("row", "col")), P()), check_vma=False
    )
```
